32 devices in a mesh: dp: 1 (over z), ch: 4 (over y), wd: 8 (over x, core).
Axes of the slice: x: 4, y: 4, z: 1, core: 2. Of those that a mesh axis runs over, the one named last changes fastest.
The devices are a block of a 4x4x8 slice.
Arguments:
- resid_in: bfloat16 [4096, 3072], P('dp', 'wd')
- seg_pos: int32 [1, 4096], P('dp')
- gain_temporal: bfloat16 [3072], P('wd')
- w_x: bfloat16 [3072, 4096], P('wd', 'ch')
- bias_x: bfloat16 [4096], P('ch')
- w_y: bfloat16 [3072, 4096], P('wd', 'ch')
- bias_y: bfloat16 [4096], P('ch')
- conv_w: bfloat16 [4, 4096], P(None, 'ch')
- conv_bias: bfloat16 [4096], P('ch')
- lam_param: float32 [4096], P('ch')
- rgate_w: bfloat16 [16, 256, 256], P('ch')
- rgate_b: bfloat16 [4096], P('ch')
- igate_w: bfloat16 [16, 256, 256], P('ch')
- igate_b: bfloat16 [4096], P('ch')
- w_o: bfloat16 [4096, 3072], P('ch', 'wd')
- bias_o: bfloat16 [3072], P('wd')
- gain_mlp: bfloat16 [3072], P('wd')
- w_g: bfloat16 [3072, 9216], P('wd', 'ch')
- bias_g: bfloat16 [9216], P('ch')
- w_u: bfloat16 [3072, 9216], P('wd', 'ch')
- bias_u: bfloat16 [9216], P('ch')
- w_d: bfloat16 [9216, 3072], P('ch', 'wd')
- bias_d: bfloat16 [3072], P('wd')
Outputs:
- output: bfloat16 [4096, 3072], P('dp', 'wd')
All inputs are finite; a program needn't handle non-finite values.
Results may differ from the reference program's by a relative error of at most 0.0128775.
Values are sent between devices in bfloat16 or wider.
A program may use at most 768 MiB of HBM per device.

```python
import jax
import jax.numpy as jnp
from jax import lax

D = 3072
D_RNN = 4096
F = 9216
BLOCKS = 16
B = 1
T = 4096
CONV_WIDTH = 4
BLOCK_WIDTH = D_RNN // BLOCKS
EPS = 1e-6


def normal_draw(key, shape, scale):
    return (jax.random.normal(key, shape, jnp.float32) * scale).astype(jnp.bfloat16)


def doc_positions(key):
    cuts = jax.random.randint(key, (B, 4), 0, T)
    steps = jnp.arange(T, dtype=jnp.int32)
    starts = jnp.any(steps[None, :, None] == cuts[:, None, :], axis=2) | (steps == 0)[None, :]
    last_start = lax.cummax(jnp.where(starts, steps[None, :], 0), axis=1)
    return (steps[None, :] - last_start).astype(jnp.int32)


def setup_inputs(seed: int = 0, part: int = 0) -> dict:
    root = jax.random.key(seed)
    part_key = jax.random.fold_in(root, part)
    keys = jax.random.split(root, 24)
    col_ramp = 0.5 + 1.5 * jnp.arange(D, dtype=jnp.float32) / D
    noise = jax.random.normal(jax.random.fold_in(part_key, 0), (B * T, D), jnp.float32)
    decay_target = jax.random.uniform(keys[9], (D_RNN,), jnp.float32, 0.9, 0.999)
    sigma_lam = decay_target ** 0.125
    return {
        'resid_in': (noise * col_ramp).astype(jnp.bfloat16),
        'seg_pos': doc_positions(jax.random.fold_in(part_key, 1)),
        'gain_temporal': normal_draw(keys[0], (D,), 0.5),
        'w_x': normal_draw(keys[1], (D, D_RNN), D ** -0.5),
        'bias_x': normal_draw(keys[2], (D_RNN,), 0.5),
        'w_y': normal_draw(keys[3], (D, D_RNN), D ** -0.5),
        'bias_y': normal_draw(keys[4], (D_RNN,), 0.5),
        'conv_w': normal_draw(keys[5], (CONV_WIDTH, D_RNN), 0.5),
        'conv_bias': normal_draw(keys[6], (D_RNN,), 0.5),
        'lam_param': jnp.log(sigma_lam / (1.0 - sigma_lam)),
        'rgate_w': normal_draw(keys[7], (BLOCKS, BLOCK_WIDTH, BLOCK_WIDTH), BLOCK_WIDTH ** -0.5),
        'rgate_b': normal_draw(keys[8], (D_RNN,), 1.0),
        'igate_w': normal_draw(keys[10], (BLOCKS, BLOCK_WIDTH, BLOCK_WIDTH), BLOCK_WIDTH ** -0.5),
        'igate_b': normal_draw(keys[11], (D_RNN,), 1.0),
        'w_o': normal_draw(keys[12], (D_RNN, D), 1.5 * D_RNN ** -0.5),
        'bias_o': normal_draw(keys[13], (D,), 0.5),
        'gain_mlp': normal_draw(keys[14], (D,), 0.5),
        'w_g': normal_draw(keys[15], (D, F), D ** -0.5),
        'bias_g': normal_draw(keys[16], (F,), 0.5),
        'w_u': normal_draw(keys[17], (D, F), D ** -0.5),
        'bias_u': normal_draw(keys[18], (F,), 0.5),
        'w_d': normal_draw(keys[19], (F, D), 1.5 * F ** -0.5),
        'bias_d': normal_draw(keys[20], (D,), 0.5),
    }


def rms_scale(vals, gain):
    mean_sq = jnp.mean(vals * vals, axis=-1, keepdims=True)
    return (vals * lax.rsqrt(mean_sq + EPS) * (1.0 + gain.astype(jnp.float32))).astype(jnp.bfloat16)


def conv_mix(vals, positions, conv_w, conv_bias):
    vals32 = vals.astype(jnp.float32)
    taps = conv_w.astype(jnp.float32)
    total = conv_bias.astype(jnp.float32) + vals32 * taps[0]
    for shift in range(1, CONV_WIDTH):
        moved = jnp.pad(vals32[:-shift], ((shift, 0), (0, 0)))
        total = total + jnp.where((positions >= shift)[:, None], moved, 0.0) * taps[shift]
    return total.astype(jnp.bfloat16)


def combine(left, right):
    return left[0] * right[0], right[0] * left[1] + right[1]


def rg_lru(conv_out, positions, lam_param, rgate_w, rgate_b, igate_w, igate_b):
    grouped = conv_out.astype(jnp.float32).reshape(T, BLOCKS, BLOCK_WIDTH)
    rate = jax.nn.sigmoid(jnp.einsum('tbi,bij->tbj', grouped, rgate_w.astype(jnp.float32)).reshape(T, D_RNN) + rgate_b.astype(jnp.float32))
    inflow = jax.nn.sigmoid(jnp.einsum('tbi,bij->tbj', grouped, igate_w.astype(jnp.float32)).reshape(T, D_RNN) + igate_b.astype(jnp.float32))
    log_a = -8.0 * rate * jax.nn.softplus(-lam_param.astype(jnp.float32))
    reset = (positions == 0)[:, None]
    decay = jnp.where(reset, 0.0, jnp.exp(log_a))
    scale = jnp.where(reset, 1.0, jnp.sqrt(-jnp.expm1(2.0 * log_a)))
    drive = scale * inflow * conv_out.astype(jnp.float32)
    return lax.associative_scan(combine, (decay, drive), axis=0)[1]


def reference(resid_in, seg_pos, gain_temporal, w_x, bias_x, w_y, bias_y, conv_w, conv_bias, lam_param, rgate_w, rgate_b, igate_w, igate_b, w_o, bias_o, gain_mlp, w_g, bias_g, w_u, bias_u, w_d, bias_d):
    def one_sequence(pair):
        seq_x, positions = pair
        resid32 = seq_x.astype(jnp.float32)
        normed = rms_scale(resid32, gain_temporal)
        y_branch = jax.nn.gelu(jnp.dot(normed, w_y, preferred_element_type=jnp.float32) + bias_y.astype(jnp.float32), approximate=True).astype(jnp.bfloat16)
        u_branch = (jnp.dot(normed, w_x, preferred_element_type=jnp.float32) + bias_x.astype(jnp.float32)).astype(jnp.bfloat16)
        conv_out = conv_mix(u_branch, positions, conv_w, conv_bias)
        hidden = rg_lru(conv_out, positions, lam_param, rgate_w, rgate_b, igate_w, igate_b)
        mixed = (hidden * y_branch.astype(jnp.float32)).astype(jnp.bfloat16)
        resid = resid32 + jnp.dot(mixed, w_o, preferred_element_type=jnp.float32) + bias_o.astype(jnp.float32)
        normed2 = rms_scale(resid, gain_mlp)
        gate = jax.nn.gelu(jnp.dot(normed2, w_g, preferred_element_type=jnp.float32) + bias_g.astype(jnp.float32), approximate=True)
        upper = jnp.dot(normed2, w_u, preferred_element_type=jnp.float32) + bias_u.astype(jnp.float32)
        inner = (gate * upper).astype(jnp.bfloat16)
        return (resid + jnp.dot(inner, w_d, preferred_element_type=jnp.float32) + bias_d.astype(jnp.float32)).astype(jnp.bfloat16)
    per_seq = lax.map(one_sequence, (resid_in.reshape(B, T, D), seg_pos))
    return per_seq.reshape(B * T, D)
```

```python
import functools

import jax
import jax.numpy as jnp
from jax import lax
from jax.experimental import pallas as pl
from jax.experimental.pallas import tpu as pltpu
from jax.sharding import PartitionSpec as P

EPS = 1e-6
F32 = jnp.float32
BF16 = jnp.bfloat16
MESH = pl.DeviceIdType.MESH
VMEM = pltpu.VMEM
ANY = pl.ANY
HALO = 16
TILE = 8
VMEM_LIMIT = 62 * 1024 * 1024
HOPS = ((0, 0), (0, 1), (-1, 0), (1, 0), (-1, 1), (1, 1), (2, 0), (2, 1))


def remote(src, dst, send, recv, **to):
    return pltpu.make_async_remote_copy(src_ref=src, dst_ref=dst, send_sem=send, recv_sem=recv, device_id=to, device_id_type=MESH)


def shifted(index, by, count):
    return lax.rem(index + (by % count), count)


def rms(vals, sum_sq, width, gain):
    return (vals * lax.rsqrt(sum_sq / width + EPS) * (1.0 + gain)).astype(BF16)


def aligned(start, size):
    return pl.ds(pl.multiple_of(start, size), size)


def ring_gather(buf, c, nc, rows, send, recv):
    right, left = shifted(c, 1, nc), shifted(c, -1, nc)
    half = rows // 2

    def make(block, part, to, k):
        piece = buf.at[aligned(block * rows + part * half, half)]
        return remote(piece, piece, send.at[k], recv.at[k], ch=to)

    own = [make(c, 0, right, 0), make(c, 1, left, 1), make(c, 1, right, 2), make(c, 0, left, 3)]
    relay = [make(left, 0, right, 4), make(right, 1, left, 5)]

    def begin():
        for copy in own:
            copy.start()

    def middle():
        for copy, onward in zip(own[:2], relay):
            copy.wait_recv()
            onward.start()

    def end():
        for copy in own[2:] + relay:
            copy.wait_recv()
        for copy in own + relay:
            copy.wait_send()

    return begin, middle, end


def ring_sums(c, nc, rows, pbuf, sbuf, far_r, far_l, near_r, near_l, send, recv):
    right, left = shifted(c, 1, nc), shifted(c, -1, nc)
    opposite = shifted(c, 2, nc)
    half = rows // 2

    def at(block, part=None):
        if part is None:
            return aligned(block * rows, rows)
        return aligned(block * rows + part * half, half)

    def far(k):
        return (remote(sbuf.at[k, at(opposite, 0)], far_r.at[k], send.at[0, k], recv.at[0, k], ch=right),
                remote(sbuf.at[k, at(opposite, 1)], far_l.at[k], send.at[1, k], recv.at[1, k], ch=left))

    def near(k):
        return (remote(sbuf.at[k, at(right)], near_r.at[k], send.at[2, k], recv.at[2, k], ch=right),
                remote(sbuf.at[k, at(left)], near_l.at[k], send.at[3, k], recv.at[3, k], ch=left))

    def first(k, partial):
        pbuf[k] = partial
        sbuf[k] = partial.astype(BF16)
        for copy in far(k):
            copy.start()

    def second(k):
        to_right, to_left = far(k)
        onward = near(k)
        to_right.wait_recv()
        sbuf[k, at(right, 0)] = (pbuf[k, at(right, 0)] + far_r[k].astype(F32)).astype(BF16)
        onward[0].start()
        to_left.wait_recv()
        sbuf[k, at(left, 1)] = (pbuf[k, at(left, 1)] + far_l[k].astype(F32)).astype(BF16)
        onward[1].start()

    def third(k):
        for copy in near(k):
            copy.wait_recv()
        return pbuf[k, at(c)] + near_r[k].astype(F32) + near_l[k].astype(F32)

    def drain(k):
        for copy in far(k) + near(k):
            copy.wait_send()

    return first, second, third, drain


def layer_kernel(nw, nc, x_ref, seg_ref, wx, wy, wo, wg, wu, wd, gt_ref, bo_ref, gm_ref, bd_ref, bx_ref, by_ref, cb_ref, rb_ref, ib_ref, lam_ref, cw_ref, rg_ref, ig_ref, bg_ref, bu_ref,
                 out_ref, wx_all, wy_all, wo_all, wg_all, wu_all, wd_all,
                 xbuf, pbufs, pv_ref, pos_ref, wide_ref, xown, pars, nall, mall, wtile, ctile, stage_r, stage_c, ubuf, hsend, hrecv, ybuf, abuf, bbuf, tot, mixed, gbuf, inner, res,
                 pbuf, sbuf, far_r, far_l, near_r, near_l, osend, fin,
                 lsem, tsem, csem, outsem, xs, xr, ps, pr, ns, nr, hs, hr, ts, tr, as_, ar, ms, mr, ds, dr, os_, or_, fs, fr, ss, rs):
    w, c = lax.axis_index('wd'), lax.axis_index('ch')
    nx = nw // 2
    chip, core = w // 2, w % 2
    rows, part = xown.shape[0], xbuf.shape[2]
    tokens, chans = ybuf.shape
    width = part * nw

    def member(step, other):
        return shifted(chip, step, nx) * 2 + (core + other) % 2

    right_w, left_w, far_w, mate = member(1, 0), member(-1, 0), member(2, 0), member(0, 1)

    barrier = pltpu.get_barrier_semaphore()
    for d in range(1, nw):
        pl.semaphore_signal(barrier, inc=1, device_id={'wd': shifted(w, d, nw)}, device_id_type=MESH)
    for d in (1, -1):
        pl.semaphore_signal(barrier, inc=1, device_id={'ch': shifted(c, d, nc)}, device_id_type=MESH)
    pl.semaphore_wait(barrier, nw + 1)

    weights = ((wx, wx_all), (wy, wy_all), (wo, wo_all), (wg, wg_all), (wu, wu_all), (wd, wd_all))

    def stream(i):
        src, dst = weights[i]
        depth = src.shape[0]
        half = depth // 2

        def piece(block, k):
            return dst.at[aligned(block * depth + k * half, half)]

        low, high = src.at[pl.ds(0, half)], src.at[pl.ds(half, half)]
        mine = dst.at[aligned(w * depth, depth)]
        first_sends = ((low, piece(w, 0), right_w), (high, piece(w, 1), left_w), (high, piece(w, 1), right_w), (low, piece(w, 0), left_w), (src, mine, mate))
        relays = ((left_w, 0, right_w), (right_w, 1, left_w), (left_w, 0, mate), (right_w, 1, mate), (left_w, 1, mate), (right_w, 0, mate), (far_w, 0, mate), (far_w, 1, mate))

        def copy(k):
            if k < len(first_sends):
                source, target, to = first_sends[k]
            else:
                block, p, to = relays[k - len(first_sends)]
                source = target = piece(block, p)
            return remote(source, target, ss.at[i, k], rs.at[i, k], wd=to)

        if depth == part:
            stage = stage_r.at[:, pl.ds(0, src.shape[1])]
        else:
            stage = stage_c.at[pl.ds(0, depth)]

        def load():
            return pltpu.make_async_copy(src, stage, lsem.at[0])

        def keep():
            return pltpu.make_async_copy(stage, mine, lsem.at[1])

        return copy, load, keep

    def send_own(i):
        copy, load, keep = stream(i)
        for k in range(5):
            copy(k).start()
        load().start()
        load().wait()
        keep().start()

    def send_on(i):
        copy, load, keep = stream(i)
        keep().wait()
        copy(0).wait_recv()
        copy(5).start()
        copy(7).start()
        copy(1).wait_recv()
        copy(6).start()
        copy(8).start()

    def send_on_and_next(i):
        send_on(i)
        send_own(i + 1)

    def ready(i):
        copy = stream(i)[0]
        for k, onward in ((2, 9), (3, 10), (5, 11), (6, 12)):
            copy(k).wait_recv()
            copy(onward).start()
        for k in (4, 7, 8, 9, 10, 11, 12):
            copy(k).wait_recv()

    def column_tiles(src, body):
        size = wtile.shape[2]
        count = src.shape[1] // size

        def load(j, slot):
            return pltpu.make_async_copy(src.at[:, aligned(j * size, size)], wtile.at[slot], tsem.at[slot])

        load(0, 0).start()

        def step(j, carry):
            slot = lax.rem(j, 2)

            @pl.when(j + 1 < count)
            def _():
                load(j + 1, 1 - slot).start()

            load(j, slot).wait()
            body(aligned(j * size, size), wtile[slot])
            return carry

        lax.fori_loop(0, count, step, 0)

    def rows_of(t):
        return x_ref.at[aligned((t * nc + c) * rows, rows)]

    def wide_row(ref):
        return ref[...].astype(F32)[None, :]

    for k, ref in enumerate((gt_ref, bo_ref, gm_ref, bd_ref)):
        pbufs[w, k:k + 1, :] = wide_row(ref)
    pbufs[w, 4:, :] = jnp.zeros((4, part), F32)
    own = pltpu.make_async_copy(rows_of(w), xbuf.at[w], lsem.at[2])
    own.start()
    copies = []
    for d in range(1, nw):
        t = shifted(w, d, nw)
        copies.append(remote(rows_of(t), xbuf.at[w], xs.at[d], xr.at[d], wd=t))
        copies.append(remote(pbufs.at[w], pbufs.at[w], ps.at[d], pr.at[d], wd=t))
    for copy in copies:
        copy.start()
    send_own(0)
    for k, ref in enumerate((bx_ref, by_ref, cb_ref, rb_ref, ib_ref)):
        pv_ref[k:k + 1, :] = wide_row(ref)
    lam = lam_ref[...][None, :]
    pv_ref[5:6, :] = -8.0 * (jnp.maximum(-lam, 0.0) + jnp.log1p(jnp.exp(-jnp.abs(lam))))
    pv_ref[6:10, :] = cw_ref[...].astype(F32)
    wide_ref[0:1, :] = wide_row(bg_ref)
    wide_ref[1:2, :] = wide_row(bu_ref)
    pos_row = seg_ref[0:1, aligned(w * tokens, tokens)].astype(F32)
    pos_cols = jnp.broadcast_to(pos_row, (128, tokens)).T.astype(jnp.int32)
    for k in range(pos_ref.shape[1] // 128):
        pos_ref[:, k * 128:(k + 1) * 128] = pos_cols
    own.wait()
    for copy in copies:
        copy.wait_recv()
    total = jnp.zeros((rows, 1), F32)
    for j in range(nw):
        vals = xbuf[j].astype(F32)
        total = total + jnp.sum(vals * vals, axis=1, keepdims=True)
    my_rows = aligned(c * rows, rows)
    for j in range(nw):
        cols = slice(j * part, (j + 1) * part)
        xown[:, cols] = xbuf[j]
        pars[:, cols] = pbufs[j]
        nall[my_rows, cols] = rms(xbuf[j].astype(F32), total, width, pbufs[j, 0:1])
    begin, middle, end = ring_gather(nall, c, nc, rows, ns, nr)
    begin()
    for copy in copies:
        copy.wait_send()
    send_on_and_next(0)
    middle()
    end()

    ready(0)

    def u_tile(cols, weight):
        u = jnp.dot(nall[...], weight, preferred_element_type=F32) + pv_ref[0:1, cols]
        ubuf[pl.ds(HALO, tokens), cols] = u.astype(BF16).astype(F32)

    column_tiles(wx_all, u_tile)
    hsend[...] = ubuf[pl.ds(tokens, HALO), :].astype(BF16)
    halo = remote(hsend, hrecv, hs.at[0], hr.at[0], wd=shifted(w, 1, nw))
    halo.start()
    send_on_and_next(1)
    ready(1)

    def y_tile(cols, weight):
        y = jnp.dot(nall[...], weight, preferred_element_type=F32) + pv_ref[1:2, cols]
        ybuf[:, cols] = jax.nn.gelu(y, approximate=True).astype(BF16)

    column_tiles(wy_all, y_tile)
    halo.wait()
    ubuf[pl.ds(0, HALO), :] = hrecv[...].astype(F32)
    blocks, bw = rg_ref.shape[0], rg_ref.shape[1]

    def gate_block(j, carry):
        cols = aligned(j * bw, bw)
        pos = pos_ref[...]
        conv = pv_ref[2:3, cols] + ubuf[pl.ds(HALO, tokens), cols] * pv_ref[6:7, cols]
        for k in range(1, 4):
            conv = conv + jnp.where(pos >= k, ubuf[pl.ds(HALO - k, tokens), cols], 0.0) * pv_ref[6 + k:7 + k, cols]
        conv = conv.astype(BF16)
        rate = jax.nn.sigmoid(jnp.dot(conv, rg_ref[j], preferred_element_type=F32) + pv_ref[3:4, cols])
        inflow = jax.nn.sigmoid(jnp.dot(conv, ig_ref[j], preferred_element_type=F32) + pv_ref[4:5, cols])
        log_a = rate * pv_ref[5:6, cols]
        a = jnp.exp(log_a)
        z = 2.0 * log_a
        series = 1.0 + z * (1.0 / 8.0)
        for k in range(7, 1, -1):
            series = 1.0 + z * series * (1.0 / k)
        gap = jnp.maximum(jnp.where(z > -0.5, -z * series, 1.0 - a * a), 0.0)
        root = jnp.where(gap > 0.0, gap * lax.rsqrt(jnp.where(gap > 0.0, gap, 1.0)), 0.0)
        reset = pos == 0
        abuf[:, cols] = jnp.where(reset, 0.0, a)
        bbuf[:, cols] = jnp.where(reset, 1.0, root) * inflow * conv.astype(F32)
        return carry

    lax.fori_loop(0, blocks, gate_block, 0)
    send_on(2)

    sub = lax.broadcasted_iota(jnp.int32, (TILE, chans), 0)

    def scan_tile(i, carry):
        a_in, h_in = carry
        at = aligned(i * TILE, TILE)
        a, b = abuf[at, :], bbuf[at, :]
        for d in (1, 2, 4):
            keep = sub >= d
            b = b + a * jnp.where(keep, pltpu.roll(b, d, 0), 0.0)
            a = a * jnp.where(keep, pltpu.roll(a, d, 0), 1.0)
        h = b + a * h_in
        a = a * a_in
        abuf[at, :] = a
        bbuf[at, :] = h
        return jnp.broadcast_to(a[TILE - 1:], a.shape), jnp.broadcast_to(h[TILE - 1:], h.shape)

    a_tot, h_tot = lax.fori_loop(0, tokens // TILE, scan_tile, (jnp.ones((TILE, chans), F32), jnp.zeros((TILE, chans), F32)))
    tot[w] = jnp.where(sub < TILE // 2, a_tot, h_tot)
    copies = []
    for d in range(1, nw):
        copies.append(remote(tot.at[w], tot.at[w], ts.at[d], tr.at[d], wd=shifted(w, d, nw)))
    for copy in copies:
        copy.start()
    send_own(3)
    for copy in copies:
        copy.wait_recv()
    h_in = jnp.zeros((1, chans), F32)
    for s in range(nw):
        h_in = jnp.where(s < w, tot[s, 0:1] * h_in + tot[s, TILE - 1:], h_in)
    for j in range(blocks):
        cols = slice(j * bw, (j + 1) * bw)
        hidden = bbuf[:, cols] + abuf[:, cols] * h_in[:, cols]
        mixed[:, cols] = (hidden * ybuf[:, cols].astype(F32)).astype(BF16)
    for copy in copies:
        copy.wait_send()

    ready(2)
    first, second, third, drain = ring_sums(c, nc, rows, pbuf, sbuf, far_r, far_l, near_r, near_l, as_, ar)

    def o_load(j, slot):
        return pltpu.make_async_copy(wo_all.at[aligned(j * chans, chans)], ctile.at[slot, pl.ds(0, chans)], csem.at[slot])

    o_load(0, 0).start()

    def o_step(k, carry):
        slot = lax.rem(k, 2)

        @pl.when(k + 1 < nw)
        def _():
            o_load(k + 1, 1 - slot).start()

        o_load(k, slot).wait()
        first(k, jnp.dot(mixed[...], ctile[slot, pl.ds(0, chans), :], preferred_element_type=F32))
        return carry

    def o_second(k, carry):
        second(k)
        return carry

    lax.fori_loop(0, nw, o_step, 0)
    lax.fori_loop(0, nw, o_second, 0)
    send_on_and_next(3)
    total = jnp.zeros((rows, 1), F32)
    for k in range(nw):
        cols = slice(k * part, (k + 1) * part)
        vals = xown[:, cols].astype(F32) + third(k) + pars[1:2, cols]
        res[:, cols] = vals
        total = total + jnp.sum(vals * vals, axis=1, keepdims=True)
    for k in range(nw):
        cols = slice(k * part, (k + 1) * part)
        mall[my_rows, cols] = rms(res[:, cols], total, width, pars[2:3, cols])
    begin, middle, end = ring_gather(mall, c, nc, rows, ms, mr)
    begin()

    def o_drain(k, carry):
        drain(k)
        return carry

    lax.fori_loop(0, nw, o_drain, 0)
    middle()
    end()

    ready(3)

    def g_tile(cols, weight):
        g = jnp.dot(mall[...], weight, preferred_element_type=F32) + wide_ref[0:1, cols]
        gbuf[:, cols] = jax.nn.gelu(g, approximate=True)

    column_tiles(wg_all, g_tile)
    send_on_and_next(4)
    ready(4)

    def i_tile(cols, weight):
        u = jnp.dot(mall[...], weight, preferred_element_type=F32) + wide_ref[1:2, cols]
        inner[:, cols] = (gbuf[:, cols] * u).astype(BF16)

    column_tiles(wu_all, i_tile)
    send_on(5)

    first, second, third, drain = ring_sums(c, nc, rows, pbuf, sbuf, far_r, far_l, near_r, near_l, ds, dr)
    right, left = shifted(c, 1, nc), shifted(c, -1, nc)
    half = rows // 2
    depth = wd.shape[0]

    def pick(d, options):
        value = options[0]
        for k in range(1, nw):
            value = jnp.where(d == k, options[k], value)
        return value

    targets = [member(step, other) for step, other in HOPS]
    sources = [member(-step, other) for step, other in HOPS]

    def block_of(d):
        return pick(d, targets)

    def source_of(d):
        return pick(d, sources)

    down = stream(5)[0]

    def arrived(d):
        needs = {1: ((4, None),), 2: ((2, 9), (3, 10)), 4: ((7, None), (9, None)), 5: ((8, None), (10, None)), 6: ((5, 11), (6, 12)), 7: ((11, None), (12, None))}
        for k, items in needs.items():
            @pl.when(d == k)
            def _():
                for index, onward in items:
                    down(index).wait_recv()
                    if onward is not None:
                        down(onward).start()

    def rows_at(owner, group, at=0, size=rows):
        return aligned((owner * nc + group) * rows + at, size)

    def hop(d):
        return remote(osend.at[d], fin.at[rows_at(w, c)], os_.at[d], or_.at[d], wd=block_of(d))

    def spread(d):
        piece = fin.at[rows_at(source_of(d), c)]
        return (remote(piece, piece, fs.at[0, d], fr.at[0, d], ch=right), remote(piece, piece, fs.at[1, d], fr.at[1, d], ch=left))

    def relay(d):
        from_left = fin.at[rows_at(source_of(d), left, 0, half)]
        from_right = fin.at[rows_at(source_of(d), right, half, half)]
        return (remote(from_left, from_left, fs.at[2, d], fr.at[2, d], ch=right), remote(from_right, from_right, fs.at[3, d], fr.at[3, d], ch=left))

    def finish(e):
        cols = aligned(block_of(e) * part, part)
        done = (res[:, cols] + third(e) + pars[3:4, cols]).astype(BF16)

        @pl.when(e == 0)
        def _():
            fin[rows_at(w, c), :] = done

        @pl.when(e > 0)
        def _():
            osend[e] = done
            hop(e).start()

    def share(e):
        @pl.when(e > 0)
        def _():
            hop(e).wait_recv()

        for copy in spread(e):
            copy.start()

    def pass_on(e):
        for copy, onward in zip(spread(e), relay(e)):
            copy.wait_recv()
            onward.start()

    def store(e):
        at = aligned(source_of(e) * tokens, tokens)
        return pltpu.make_async_copy(fin.at[at], out_ref.at[at], outsem.at[e])

    def complete(e):
        for copy in relay(e):
            copy.wait_recv()
        store(e).start()

    def d_step(d, carry):
        arrived(d)
        load = pltpu.make_async_copy(wd_all.at[aligned(block_of(d) * depth, depth)], ctile.at[0], csem.at[0])
        load.start()
        load.wait()
        first(d, jnp.dot(inner[...], ctile[0], preferred_element_type=F32))

        @pl.when(d >= 1)
        def _():
            second(d - 1)

        @pl.when(d >= 2)
        def _():
            finish(d - 2)

        for k in (0, 1):
            @pl.when(d == k + 4)
            def _():
                share(k)

            @pl.when(d == k + 6)
            def _():
                pass_on(k)

        return carry

    def each(first_one, last_one, body):
        def step(e, carry):
            body(e)
            return carry

        lax.fori_loop(first_one, last_one, step, 0)

    lax.fori_loop(0, nw, d_step, 0)
    second(nw - 1)
    finish(nw - 2)
    each(2, 4, share)
    finish(nw - 1)
    each(4, 6, share)
    each(2, 4, pass_on)
    share(6)
    each(4, 6, pass_on)
    share(7)
    each(6, 8, pass_on)
    each(0, nw, complete)

    def settle(d):
        for copy in spread(d) + relay(d):
            copy.wait_send()
        drain(d)

        @pl.when(d > 0)
        def _():
            hop(d).wait_send()

    each(0, nw, settle)
    for i in range(len(weights)):
        copy = stream(i)[0]
        for k in range(13):
            copy(k).wait_send()
    for k in range(nw):
        store(k).wait()


def dma(*shape):
    return pltpu.SemaphoreType.DMA(shape)


def solution(mesh):
    nw = mesh.shape['wd']
    nc = mesh.shape['ch']
    assert nc == 4 and nw == len(HOPS)
    row_spec = P('dp', 'wd')
    specs = (row_spec, P('dp', None), P('wd'), P('wd', 'ch'), P('ch'), P('wd', 'ch'), P('ch'), P(None, 'ch'), P('ch'), P('ch'), P('ch', None, None), P('ch'), P('ch', None, None), P('ch'), P('ch', 'wd'), P('wd'), P('wd'), P('wd', 'ch'), P('ch'), P('wd', 'ch'), P('ch'), P('ch', 'wd'), P('wd'))
    vm = pl.BlockSpec(memory_space=VMEM)
    anywhere = pl.BlockSpec(memory_space=ANY)

    def local_layer(resid_in, seg_pos, gain_temporal, w_x, bias_x, w_y, bias_y, conv_w, conv_bias, lam_param, rgate_w, rgate_b, igate_w, igate_b, w_o, bias_o, gain_mlp, w_g, bias_g, w_u, bias_u, w_d, bias_d):
        tokens, part = resid_in.shape
        width = part * nw
        span = tokens // nw
        rows = span // nc
        chans = w_x.shape[1]
        wide = w_g.shape[1]
        bw = rgate_w.shape[1]
        assert seg_pos.shape[0] == 1

        def landing(arr):
            return jax.ShapeDtypeStruct((arr.shape[0] * nw, arr.shape[1]), arr.dtype)

        stream = (w_x, w_y, w_o, w_g, w_u, w_d)
        scratch = [
            VMEM((nw, rows, part), BF16), VMEM((nw, 8, part), F32), VMEM((16, chans), F32), VMEM((span, bw), jnp.int32), VMEM((8, wide), F32), VMEM((rows, width), BF16), VMEM((8, width), F32),
            VMEM((span, width), BF16), VMEM((span, width), BF16), VMEM((2, width, bw), BF16), VMEM((2, wide, part), BF16),
            VMEM((part, wide), BF16), VMEM((wide, part), BF16),
            VMEM((span + HALO, chans), F32), VMEM((HALO, chans), BF16), VMEM((HALO, chans), BF16), VMEM((span, chans), BF16),
            VMEM((span, chans), F32), VMEM((span, chans), F32), VMEM((nw, TILE, chans), F32), VMEM((span, chans), BF16),
            VMEM((span, wide), F32), VMEM((span, wide), BF16), VMEM((rows, width), F32),
            VMEM((nw, span, part), F32), VMEM((nw, span, part), BF16), VMEM((nw, rows // 2, part), BF16), VMEM((nw, rows // 2, part), BF16),
            VMEM((nw, rows, part), BF16), VMEM((nw, rows, part), BF16), VMEM((nw, rows, part), BF16), VMEM((tokens, part), BF16),
            dma(4), dma(2), dma(2), dma(nw), dma(nw), dma(nw), dma(nw), dma(nw), dma(6), dma(6), dma(1), dma(1), dma(nw), dma(nw),
            dma(4, nw), dma(4, nw), dma(6), dma(6), dma(4, nw), dma(4, nw), dma(nw), dma(nw), dma(4, nw), dma(4, nw),
            dma(len(stream), 13), dma(len(stream), 13),
        ]
        return pl.pallas_call(
            functools.partial(layer_kernel, nw, nc), name='layer',
            out_shape=(jax.ShapeDtypeStruct((tokens, part), BF16),) + tuple(landing(arr) for arr in stream),
            in_specs=[anywhere] + [vm] + [anywhere] * 6 + [vm] * 15, out_specs=(anywhere,) * 7, scratch_shapes=scratch,
            compiler_params=pltpu.CompilerParams(vmem_limit_bytes=VMEM_LIMIT, collective_id=0, has_side_effects=True),
        )(resid_in, seg_pos, *stream, gain_temporal, bias_o, gain_mlp, bias_d, bias_x, bias_y, conv_bias, rgate_b, igate_b, lam_param, conv_w, rgate_w, igate_w, bias_g, bias_u)[0]

    return jax.shard_map(local_layer, mesh=mesh, in_specs=specs, out_specs=row_spec, check_vma=False)
```

```python
import functools

import jax
import jax.numpy as jnp
from jax import lax
from jax.experimental import pallas as pl
from jax.experimental.pallas import tpu as pltpu
from jax.sharding import PartitionSpec as P

EPS = 1e-6
SLIM = 128
F32 = jnp.float32
BF16 = jnp.bfloat16
MESH = pl.DeviceIdType.MESH
VMEM = pltpu.VMEM
ANY = pl.ANY
HALO = 16
TILE = 8
VMEM_LIMIT = 62 * 1024 * 1024
HOPS = ((0, 0), (0, 1), (-1, 0), (1, 0), (-1, 1), (1, 1), (2, 0), (2, 1))


def remote(src, dst, send, recv, **to):
    return pltpu.make_async_remote_copy(src_ref=src, dst_ref=dst, send_sem=send, recv_sem=recv, device_id=to, device_id_type=MESH)


def shifted(index, by, count):
    return lax.rem(index + (by % count), count)


def rms(vals, sum_sq, width, gain):
    return (vals * lax.rsqrt(sum_sq / width + EPS) * (1.0 + gain)).astype(BF16)


def aligned(start, size):
    return pl.ds(pl.multiple_of(start, size), size)


def ring_gather(buf, c, nc, rows, send, recv):
    right, left = shifted(c, 1, nc), shifted(c, -1, nc)
    half = rows // 2

    def make(block, part, to, k):
        piece = buf.at[aligned(block * rows + part * half, half)]
        return remote(piece, piece, send.at[k], recv.at[k], ch=to)

    own = [make(c, 0, right, 0), make(c, 1, left, 1), make(c, 1, right, 2), make(c, 0, left, 3)]
    relay = [make(left, 0, right, 4), make(right, 1, left, 5)]

    def begin():
        for copy in own:
            copy.start()

    def middle():
        for copy, onward in zip(own[:2], relay):
            copy.wait_recv()
            onward.start()

    def end():
        for copy in own[2:] + relay:
            copy.wait_recv()
        for copy in own + relay:
            copy.wait_send()

    return begin, middle, end


def ring_sums(c, nc, rows, pbuf, sbuf, far_r, far_l, near_r, near_l, send, recv):
    right, left = shifted(c, 1, nc), shifted(c, -1, nc)
    opposite = shifted(c, 2, nc)
    half = rows // 2

    def at(block, part=None):
        if part is None:
            return aligned(block * rows, rows)
        return aligned(block * rows + part * half, half)

    def far(unit):
        k, s, lanes = unit
        return (remote(sbuf.at[k, at(opposite, 0), lanes], far_r.at[k, :, lanes], send.at[0, s], recv.at[0, s], ch=right),
                remote(sbuf.at[k, at(opposite, 1), lanes], far_l.at[k, :, lanes], send.at[1, s], recv.at[1, s], ch=left))

    def near(unit):
        k, s, lanes = unit
        return (remote(sbuf.at[k, at(right), lanes], near_r.at[k, :, lanes], send.at[2, s], recv.at[2, s], ch=right),
                remote(sbuf.at[k, at(left), lanes], near_l.at[k, :, lanes], send.at[3, s], recv.at[3, s], ch=left))

    def first(unit, partial):
        k, s, lanes = unit
        pbuf[k, :, lanes] = partial
        sbuf[k, :, lanes] = partial.astype(BF16)
        for copy in far(unit):
            copy.start()

    def second(unit):
        k, s, lanes = unit
        to_right, to_left = far(unit)
        onward = near(unit)
        to_right.wait_recv()
        sbuf[k, at(right, 0), lanes] = (pbuf[k, at(right, 0), lanes] + far_r[k, :, lanes].astype(F32)).astype(BF16)
        onward[0].start()
        to_left.wait_recv()
        sbuf[k, at(left, 1), lanes] = (pbuf[k, at(left, 1), lanes] + far_l[k, :, lanes].astype(F32)).astype(BF16)
        onward[1].start()

    def third(unit):
        k, s, lanes = unit
        for copy in near(unit):
            copy.wait_recv()
        return pbuf[k, at(c), lanes] + near_r[k, :, lanes].astype(F32) + near_l[k, :, lanes].astype(F32)

    def drain(unit):
        for copy in far(unit) + near(unit):
            copy.wait_send()

    return first, second, third, drain


def layer_kernel(nw, nc, x_ref, seg_ref, wx, wy, wo, wg, wu, wd, gt_ref, bo_ref, gm_ref, bd_ref, bx_ref, by_ref, cb_ref, rb_ref, ib_ref, lam_ref, cw_ref, rg_ref, ig_ref, bg_ref, bu_ref,
                 out_ref, wx_all, wy_all, wo_all, wg_all, wu_all, wd_all,
                 xbuf, pbufs, pv_ref, pos_ref, wide_ref, xown, pars, nall, mall, wtile, ctile, stage_r, stage_c, ubuf, hsend, hrecv, ybuf, abuf, bbuf, tot, mixed, gbuf, inner, res,
                 pbuf, sbuf, far_r, far_l, near_r, near_l, osend, fin,
                 lsem, tsem, csem, outsem, xs, xr, ps, pr, ns, nr, hs, hr, ts, tr, as_, ar, ms, mr, ds, dr, os_, or_, fs, fr, ss, rs, ws, wr):
    w, c = lax.axis_index('wd'), lax.axis_index('ch')
    nx = nw // 2
    chip, core = w // 2, w % 2
    rows, part = xown.shape[0], xbuf.shape[2]
    tokens, chans = ybuf.shape
    width = part * nw
    slims = part // SLIM

    def member(step, other):
        return shifted(chip, step, nx) * 2 + (core + other) % 2

    right_w, left_w, far_w, mate = member(1, 0), member(-1, 0), member(2, 0), member(0, 1)

    barrier = pltpu.get_barrier_semaphore()
    for d in range(1, nw):
        pl.semaphore_signal(barrier, inc=1, device_id={'wd': shifted(w, d, nw)}, device_id_type=MESH)
    for d in (1, -1):
        pl.semaphore_signal(barrier, inc=1, device_id={'ch': shifted(c, d, nc)}, device_id_type=MESH)
    pl.semaphore_wait(barrier, nw + 1)

    weights = ((wx, wx_all), (wy, wy_all), (wo, wo_all), (wg, wg_all), (wu, wu_all), (wd, wd_all))

    def stream(i):
        src, dst = weights[i]
        depth = src.shape[0]
        half = depth // 2

        def piece(block, k):
            return dst.at[aligned(block * depth + k * half, half)]

        low, high = src.at[pl.ds(0, half)], src.at[pl.ds(half, half)]
        mine = dst.at[aligned(w * depth, depth)]
        first_sends = ((low, piece(w, 0), right_w), (high, piece(w, 1), left_w), (high, piece(w, 1), right_w), (low, piece(w, 0), left_w), (src, mine, mate))
        relays = ((left_w, 0, right_w), (right_w, 1, left_w), (left_w, 0, mate), (right_w, 1, mate), (left_w, 1, mate), (right_w, 0, mate), (far_w, 0, mate), (far_w, 1, mate))

        def copy(k):
            if k < len(first_sends):
                source, target, to = first_sends[k]
            else:
                block, p, to = relays[k - len(first_sends)]
                source = target = piece(block, p)
            return remote(source, target, ss.at[i, k], rs.at[i, k], wd=to)

        if depth == part:
            stage = stage_r.at[:, pl.ds(0, src.shape[1])]
        else:
            stage = stage_c.at[pl.ds(0, depth)]

        def load():
            return pltpu.make_async_copy(src, stage, lsem.at[0])

        def keep():
            return pltpu.make_async_copy(stage, mine, lsem.at[1])

        def slim(kind, t):
            block, p, to = relays[(0, 1, 6, 7)[kind]]
            rows_of_piece = piece(block, p).at[:, aligned(t * SLIM, SLIM)]
            return remote(rows_of_piece, rows_of_piece, ws.at[kind, t], wr.at[kind, t], wd=to)

        return copy, load, keep, slim

    def send_own(i):
        copy, load, keep, slim = stream(i)
        for k in range(5):
            copy(k).start()
        load().start()
        load().wait()
        keep().start()

    def send_on(i):
        copy, load, keep, slim = stream(i)
        keep().wait()
        last = i + 1 == len(weights)
        for k in range(2):
            copy(k).wait_recv()
            if last:
                for t in range(slims - 1):
                    slim(k, t).start()
            else:
                copy(5 + k).start()
            copy(7 + k).start()

    def send_on_and_next(i):
        send_on(i)
        send_own(i + 1)

    def ready(i):
        copy = stream(i)[0]
        for k, onward in ((2, 9), (3, 10), (5, 11), (6, 12)):
            copy(k).wait_recv()
            copy(onward).start()
        for k in (4, 7, 8, 9, 10, 11, 12):
            copy(k).wait_recv()

    def column_tiles(src, body):
        size = wtile.shape[2]
        count = src.shape[1] // size

        def load(j, slot):
            return pltpu.make_async_copy(src.at[:, aligned(j * size, size)], wtile.at[slot], tsem.at[slot])

        load(0, 0).start()

        def step(j, carry):
            slot = lax.rem(j, 2)

            @pl.when(j + 1 < count)
            def _():
                load(j + 1, 1 - slot).start()

            load(j, slot).wait()
            body(aligned(j * size, size), wtile[slot])
            return carry

        lax.fori_loop(0, count, step, 0)

    def rows_of(t):
        return x_ref.at[aligned((t * nc + c) * rows, rows)]

    def wide_row(ref):
        return ref[...].astype(F32)[None, :]

    for k, ref in enumerate((gt_ref, bo_ref, gm_ref, bd_ref)):
        pbufs[w, k:k + 1, :] = wide_row(ref)
    pbufs[w, 4:, :] = jnp.zeros((4, part), F32)
    own = pltpu.make_async_copy(rows_of(w), xbuf.at[w], lsem.at[2])
    own.start()
    copies = []
    for d in range(1, nw):
        t = shifted(w, d, nw)
        copies.append(remote(rows_of(t), xbuf.at[w], xs.at[d], xr.at[d], wd=t))
        copies.append(remote(pbufs.at[w], pbufs.at[w], ps.at[d], pr.at[d], wd=t))
    for copy in copies:
        copy.start()
    send_own(0)
    for k, ref in enumerate((bx_ref, by_ref, cb_ref, rb_ref, ib_ref)):
        pv_ref[k:k + 1, :] = wide_row(ref)
    lam = lam_ref[...][None, :]
    pv_ref[5:6, :] = -8.0 * (jnp.maximum(-lam, 0.0) + jnp.log1p(jnp.exp(-jnp.abs(lam))))
    pv_ref[6:10, :] = cw_ref[...].astype(F32)
    wide_ref[0:1, :] = wide_row(bg_ref)
    wide_ref[1:2, :] = wide_row(bu_ref)
    pos_row = seg_ref[0:1, aligned(w * tokens, tokens)].astype(F32)
    pos_cols = jnp.broadcast_to(pos_row, (128, tokens)).T.astype(jnp.int32)
    for k in range(pos_ref.shape[1] // 128):
        pos_ref[:, k * 128:(k + 1) * 128] = pos_cols
    own.wait()
    for copy in copies:
        copy.wait_recv()
    total = jnp.zeros((rows, 1), F32)
    for j in range(nw):
        vals = xbuf[j].astype(F32)
        total = total + jnp.sum(vals * vals, axis=1, keepdims=True)
    my_rows = aligned(c * rows, rows)
    for j in range(nw):
        cols = slice(j * part, (j + 1) * part)
        xown[:, cols] = xbuf[j]
        pars[:, cols] = pbufs[j]
        nall[my_rows, cols] = rms(xbuf[j].astype(F32), total, width, pbufs[j, 0:1])
    begin, middle, end = ring_gather(nall, c, nc, rows, ns, nr)
    begin()
    for copy in copies:
        copy.wait_send()
    send_on_and_next(0)
    middle()
    end()

    ready(0)

    def u_tile(cols, weight):
        u = jnp.dot(nall[...], weight, preferred_element_type=F32) + pv_ref[0:1, cols]
        ubuf[pl.ds(HALO, tokens), cols] = u.astype(BF16).astype(F32)

    column_tiles(wx_all, u_tile)
    hsend[...] = ubuf[pl.ds(tokens, HALO), :].astype(BF16)
    halo = remote(hsend, hrecv, hs.at[0], hr.at[0], wd=shifted(w, 1, nw))
    halo.start()
    send_on_and_next(1)
    ready(1)

    def y_tile(cols, weight):
        y = jnp.dot(nall[...], weight, preferred_element_type=F32) + pv_ref[1:2, cols]
        ybuf[:, cols] = jax.nn.gelu(y, approximate=True).astype(BF16)

    column_tiles(wy_all, y_tile)
    halo.wait()
    ubuf[pl.ds(0, HALO), :] = hrecv[...].astype(F32)
    blocks, bw = rg_ref.shape[0], rg_ref.shape[1]

    def gate_block(j, carry):
        cols = aligned(j * bw, bw)
        pos = pos_ref[...]
        conv = pv_ref[2:3, cols] + ubuf[pl.ds(HALO, tokens), cols] * pv_ref[6:7, cols]
        for k in range(1, 4):
            conv = conv + jnp.where(pos >= k, ubuf[pl.ds(HALO - k, tokens), cols], 0.0) * pv_ref[6 + k:7 + k, cols]
        conv = conv.astype(BF16)
        rate = jax.nn.sigmoid(jnp.dot(conv, rg_ref[j], preferred_element_type=F32) + pv_ref[3:4, cols])
        inflow = jax.nn.sigmoid(jnp.dot(conv, ig_ref[j], preferred_element_type=F32) + pv_ref[4:5, cols])
        log_a = rate * pv_ref[5:6, cols]
        a = jnp.exp(log_a)
        z = 2.0 * log_a
        series = 1.0 + z * (1.0 / 8.0)
        for k in range(7, 1, -1):
            series = 1.0 + z * series * (1.0 / k)
        gap = jnp.maximum(jnp.where(z > -0.5, -z * series, 1.0 - a * a), 0.0)
        root = jnp.where(gap > 0.0, gap * lax.rsqrt(jnp.where(gap > 0.0, gap, 1.0)), 0.0)
        reset = pos == 0
        abuf[:, cols] = jnp.where(reset, 0.0, a)
        bbuf[:, cols] = jnp.where(reset, 1.0, root) * inflow * conv.astype(F32)
        return carry

    lax.fori_loop(0, blocks, gate_block, 0)
    send_on(2)

    sub = lax.broadcasted_iota(jnp.int32, (TILE, chans), 0)

    def scan_tile(i, carry):
        a_in, h_in = carry
        at = aligned(i * TILE, TILE)
        a, b = abuf[at, :], bbuf[at, :]
        for d in (1, 2, 4):
            keep = sub >= d
            b = b + a * jnp.where(keep, pltpu.roll(b, d, 0), 0.0)
            a = a * jnp.where(keep, pltpu.roll(a, d, 0), 1.0)
        h = b + a * h_in
        a = a * a_in
        abuf[at, :] = a
        bbuf[at, :] = h
        return jnp.broadcast_to(a[TILE - 1:], a.shape), jnp.broadcast_to(h[TILE - 1:], h.shape)

    a_tot, h_tot = lax.fori_loop(0, tokens // TILE, scan_tile, (jnp.ones((TILE, chans), F32), jnp.zeros((TILE, chans), F32)))
    tot[w] = jnp.where(sub < TILE // 2, a_tot, h_tot)
    copies = []
    for d in range(1, nw):
        copies.append(remote(tot.at[w], tot.at[w], ts.at[d], tr.at[d], wd=shifted(w, d, nw)))
    for copy in copies:
        copy.start()
    send_own(3)
    for copy in copies:
        copy.wait_recv()
    h_in = jnp.zeros((1, chans), F32)
    for s in range(nw):
        h_in = jnp.where(s < w, tot[s, 0:1] * h_in + tot[s, TILE - 1:], h_in)
    for j in range(blocks):
        cols = slice(j * bw, (j + 1) * bw)
        hidden = bbuf[:, cols] + abuf[:, cols] * h_in[:, cols]
        mixed[:, cols] = (hidden * ybuf[:, cols].astype(F32)).astype(BF16)
    for copy in copies:
        copy.wait_send()

    ready(2)
    first, second, third, drain = ring_sums(c, nc, rows, pbuf, sbuf, far_r, far_l, near_r, near_l, as_, ar)

    def whole(k):
        return k, k, pl.ds(0, part)

    def o_load(j, slot):
        return pltpu.make_async_copy(wo_all.at[aligned(j * chans, chans)], ctile.at[slot, pl.ds(0, chans)], csem.at[slot])

    o_load(0, 0).start()

    def o_step(k, carry):
        slot = lax.rem(k, 2)

        @pl.when(k + 1 < nw)
        def _():
            o_load(k + 1, 1 - slot).start()

        o_load(k, slot).wait()
        first(whole(k), jnp.dot(mixed[...], ctile[slot, pl.ds(0, chans), :], preferred_element_type=F32))
        return carry

    def o_second(k, carry):
        second(whole(k))
        return carry

    lax.fori_loop(0, nw, o_step, 0)
    lax.fori_loop(0, nw, o_second, 0)
    send_on_and_next(3)
    total = jnp.zeros((rows, 1), F32)
    for k in range(nw):
        cols = slice(k * part, (k + 1) * part)
        vals = xown[:, cols].astype(F32) + third(whole(k)) + pars[1:2, cols]
        res[:, cols] = vals
        total = total + jnp.sum(vals * vals, axis=1, keepdims=True)
    for k in range(nw):
        cols = slice(k * part, (k + 1) * part)
        mall[my_rows, cols] = rms(res[:, cols], total, width, pars[2:3, cols])
    begin, middle, end = ring_gather(mall, c, nc, rows, ms, mr)
    begin()

    def o_drain(k, carry):
        drain(whole(k))
        return carry

    lax.fori_loop(0, nw, o_drain, 0)
    middle()
    end()

    ready(3)

    def g_tile(cols, weight):
        g = jnp.dot(mall[...], weight, preferred_element_type=F32) + wide_ref[0:1, cols]
        gbuf[:, cols] = jax.nn.gelu(g, approximate=True)

    column_tiles(wg_all, g_tile)
    send_on_and_next(4)
    ready(4)

    def i_tile(cols, weight):
        u = jnp.dot(mall[...], weight, preferred_element_type=F32) + wide_ref[1:2, cols]
        inner[:, cols] = (gbuf[:, cols] * u).astype(BF16)

    column_tiles(wu_all, i_tile)
    send_on(5)

    first, second, third, drain = ring_sums(c, nc, rows, pbuf, sbuf, far_r, far_l, near_r, near_l, ds, dr)
    right, left = shifted(c, 1, nc), shifted(c, -1, nc)
    half = rows // 2
    depth = wd.shape[0]

    def pick(d, options):
        value = options[0]
        for k in range(1, nw):
            value = jnp.where(d == k, options[k], value)
        return value

    targets = [member(step, other) for step, other in HOPS]
    sources = [member(-step, other) for step, other in HOPS]

    def block_of(d):
        return pick(d, targets)

    def source_of(d):
        return pick(d, sources)

    down, _, _, slim = stream(5)

    def arrived(d):
        needs = {1: ((4, None),), 2: ((2, 9), (3, 10)), 4: ((7, None), (9, None)), 5: ((8, None), (10, None))}
        for k, items in needs.items():
            @pl.when(d == k)
            def _():
                for index, onward in items:
                    down(index).wait_recv()
                    if onward is not None:
                        down(onward).start()

    def rows_at(owner, group, at=0, size=rows):
        return aligned((owner * nc + group) * rows + at, size)

    def hop(unit):
        d, s, lanes = unit
        return remote(osend.at[d, :, lanes], fin.at[rows_at(w, c), lanes], os_.at[s], or_.at[s], wd=block_of(d))

    def spread(unit):
        d, s, lanes = unit
        piece = fin.at[rows_at(source_of(d), c), lanes]
        return (remote(piece, piece, fs.at[0, s], fr.at[0, s], ch=right), remote(piece, piece, fs.at[1, s], fr.at[1, s], ch=left))

    def relay(unit):
        d, s, lanes = unit
        from_left = fin.at[rows_at(source_of(d), left, 0, half), lanes]
        from_right = fin.at[rows_at(source_of(d), right, half, half), lanes]
        return (remote(from_left, from_left, fs.at[2, s], fr.at[2, s], ch=right), remote(from_right, from_right, fs.at[3, s], fr.at[3, s], ch=left))

    def multiply(unit):
        d, s, lanes = unit
        target = ctile.at[0, :, lanes]
        load = pltpu.make_async_copy(wd_all.at[aligned(block_of(d) * depth, depth), lanes], target, csem.at[0])
        load.start()
        load.wait()
        first(unit, jnp.dot(inner[...], target[...], preferred_element_type=F32))

    def finish(unit):
        e, s, lanes = unit
        cols = pl.ds(pl.multiple_of(block_of(e) * part + lanes.start, SLIM), lanes.size)
        done = (res[:, cols] + third(unit) + pars[3:4, cols]).astype(BF16)

        @pl.when(e == 0)
        def _():
            fin[rows_at(w, c), lanes] = done

        @pl.when(e > 0)
        def _():
            osend[e, :, lanes] = done
            hop(unit).start()

    def share(unit):
        @pl.when(unit[0] > 0)
        def _():
            hop(unit).wait_recv()

        for copy in spread(unit):
            copy.start()

    def pass_on(unit):
        for copy, onward in zip(spread(unit), relay(unit)):
            copy.wait_recv()
            onward.start()

    def store(unit):
        e, s, lanes = unit
        at = aligned(source_of(e) * tokens, tokens)
        return pltpu.make_async_copy(fin.at[at, lanes], out_ref.at[at, lanes], outsem.at[s])

    def complete(unit):
        for copy in relay(unit):
            copy.wait_recv()
        store(unit).start()

    def settle(unit):
        for copy in spread(unit) + relay(unit):
            copy.wait_send()
        drain(unit)

        @pl.when(unit[0] > 0)
        def _():
            hop(unit).wait_send()

        store(unit).wait()

    def each(first_one, last_one, body):
        def step(e, carry):
            body(whole(e))
            return carry

        lax.fori_loop(first_one, last_one, step, 0)

    fulls = nw - 2

    def slim_units(t):
        return [(fulls + k, fulls + 2 * t + k, pl.ds(t * SLIM, SLIM)) for k in range(2)]

    def d_step(d, carry):
        arrived(d)
        multiply(whole(d))

        @pl.when(d >= 1)
        def _():
            second(whole(d - 1))

        @pl.when(d >= 2)
        def _():
            finish(whole(d - 2))

        for k in (0, 1):
            @pl.when(d == k + 4)
            def _():
                share(whole(k))

        return carry

    lax.fori_loop(0, fulls, d_step, 0)
    for k in range(2):
        slim(k, slims - 1).start()

    def slim_step(t):
        for k in range(2):
            slim(k, t).wait_recv()
            slim(2 + k, t).start()
        same, other = slim_units(t)
        multiply(same)
        for k in range(2):
            slim(2 + k, t).wait_recv()
        multiply(other)

    def do(body, t):
        for unit in slim_units(t):
            body(unit)

    slim_step(0)
    second(whole(fulls - 1))
    finish(whole(fulls - 2))
    each(0, 2, pass_on)
    for t in range(1, slims):
        slim_step(t)
        do(second, t - 1)
        if t == 1:
            finish(whole(fulls - 1))
        else:
            do(finish, t - 2)
    do(second, slims - 1)
    each(2, 4, share)
    do(finish, slims - 2)
    each(4, 6, share)
    each(2, 4, pass_on)
    do(finish, slims - 1)
    do(share, 0)
    each(4, 6, pass_on)
    for t in range(1, slims):
        do(share, t)
        do(pass_on, t - 1)
    each(0, fulls, complete)
    for t in range(slims - 1):
        do(complete, t)
    do(pass_on, slims - 1)
    do(complete, slims - 1)
    each(0, fulls, settle)
    for t in range(slims):
        do(settle, t)
    for i in range(len(weights)):
        copy, _, _, slim = stream(i)
        last = i + 1 == len(weights)
        for k in range(13):
            if not (last and k in (5, 6, 11, 12)):
                copy(k).wait_send()
        if last:
            for kind in range(4):
                for t in range(slims):
                    slim(kind, t).wait_send()


def dma(*shape):
    return pltpu.SemaphoreType.DMA(shape)


def solution(mesh):
    nw = mesh.shape['wd']
    nc = mesh.shape['ch']
    assert nc == 4 and nw == len(HOPS)
    row_spec = P('dp', 'wd')
    specs = (row_spec, P('dp', None), P('wd'), P('wd', 'ch'), P('ch'), P('wd', 'ch'), P('ch'), P(None, 'ch'), P('ch'), P('ch'), P('ch', None, None), P('ch'), P('ch', None, None), P('ch'), P('ch', 'wd'), P('wd'), P('wd'), P('wd', 'ch'), P('ch'), P('wd', 'ch'), P('ch'), P('ch', 'wd'), P('wd'))
    vm = pl.BlockSpec(memory_space=VMEM)
    anywhere = pl.BlockSpec(memory_space=ANY)

    def local_layer(resid_in, seg_pos, gain_temporal, w_x, bias_x, w_y, bias_y, conv_w, conv_bias, lam_param, rgate_w, rgate_b, igate_w, igate_b, w_o, bias_o, gain_mlp, w_g, bias_g, w_u, bias_u, w_d, bias_d):
        tokens, part = resid_in.shape
        width = part * nw
        span = tokens // nw
        rows = span // nc
        chans = w_x.shape[1]
        wide = w_g.shape[1]
        bw = rgate_w.shape[1]
        assert seg_pos.shape[0] == 1

        def landing(arr):
            return jax.ShapeDtypeStruct((arr.shape[0] * nw, arr.shape[1]), arr.dtype)

        slims = part // SLIM
        units = nw - 2 + 2 * slims
        stream = (w_x, w_y, w_o, w_g, w_u, w_d)
        scratch = [
            VMEM((nw, rows, part), BF16), VMEM((nw, 8, part), F32), VMEM((16, chans), F32), VMEM((span, bw), jnp.int32), VMEM((8, wide), F32), VMEM((rows, width), BF16), VMEM((8, width), F32),
            VMEM((span, width), BF16), VMEM((span, width), BF16), VMEM((2, width, bw), BF16), VMEM((2, wide, part), BF16),
            VMEM((part, wide), BF16), VMEM((wide, part), BF16),
            VMEM((span + HALO, chans), F32), VMEM((HALO, chans), BF16), VMEM((HALO, chans), BF16), VMEM((span, chans), BF16),
            VMEM((span, chans), F32), VMEM((span, chans), F32), VMEM((nw, TILE, chans), F32), VMEM((span, chans), BF16),
            VMEM((span, wide), F32), VMEM((span, wide), BF16), VMEM((rows, width), F32),
            VMEM((nw, span, part), F32), VMEM((nw, span, part), BF16), VMEM((nw, rows // 2, part), BF16), VMEM((nw, rows // 2, part), BF16),
            VMEM((nw, rows, part), BF16), VMEM((nw, rows, part), BF16), VMEM((nw, rows, part), BF16), VMEM((tokens, part), BF16),
            dma(4), dma(2), dma(2), dma(units), dma(nw), dma(nw), dma(nw), dma(nw), dma(6), dma(6), dma(1), dma(1), dma(nw), dma(nw),
            dma(4, nw), dma(4, nw), dma(6), dma(6), dma(4, units), dma(4, units), dma(units), dma(units), dma(4, units), dma(4, units),
            dma(len(stream), 13), dma(len(stream), 13), dma(4, slims), dma(4, slims),
        ]
        return pl.pallas_call(
            functools.partial(layer_kernel, nw, nc), name='layer',
            out_shape=(jax.ShapeDtypeStruct((tokens, part), BF16),) + tuple(landing(arr) for arr in stream),
            in_specs=[anywhere] + [vm] + [anywhere] * 6 + [vm] * 15, out_specs=(anywhere,) * 7, scratch_shapes=scratch,
            compiler_params=pltpu.CompilerParams(vmem_limit_bytes=VMEM_LIMIT, collective_id=0, has_side_effects=True),
        )(resid_in, seg_pos, *stream, gain_temporal, bias_o, gain_mlp, bias_d, bias_x, bias_y, conv_bias, rgate_b, igate_b, lam_param, conv_w, rgate_w, igate_w, bias_g, bias_u)[0]

    return jax.shard_map(local_layer, mesh=mesh, in_specs=specs, out_specs=row_spec, check_vma=False)
```

```python
import functools

import jax
import jax.numpy as jnp
from jax import lax
from jax.experimental import pallas as pl
from jax.experimental.pallas import tpu as pltpu
from jax.sharding import PartitionSpec as P

EPS = 1e-6
PIECES = 3
F32 = jnp.float32
BF16 = jnp.bfloat16
MESH = pl.DeviceIdType.MESH
VMEM = pltpu.VMEM
ANY = pl.ANY
HALO = 16
TILE = 8
VMEM_LIMIT = 62 * 1024 * 1024
HOPS = ((0, 0), (0, 1), (-1, 0), (1, 0), (-1, 1), (1, 1), (2, 0), (2, 1))


def remote(src, dst, send, recv, **to):
    return pltpu.make_async_remote_copy(src_ref=src, dst_ref=dst, send_sem=send, recv_sem=recv, device_id=to, device_id_type=MESH)


def shifted(index, by, count):
    return lax.rem(index + (by % count), count)


def rms(vals, sum_sq, width, gain):
    return (vals * lax.rsqrt(sum_sq / width + EPS) * (1.0 + gain)).astype(BF16)


def aligned(start, size):
    return pl.ds(pl.multiple_of(start, size), size)


def ring_gather(buf, c, nc, rows, send, recv):
    right, left = shifted(c, 1, nc), shifted(c, -1, nc)
    half = rows // 2

    def make(block, part, to, k):
        piece = buf.at[aligned(block * rows + part * half, half)]
        return remote(piece, piece, send.at[k], recv.at[k], ch=to)

    own = [make(c, 0, right, 0), make(c, 1, left, 1), make(c, 1, right, 2), make(c, 0, left, 3)]
    relay = [make(left, 0, right, 4), make(right, 1, left, 5)]

    def begin():
        for copy in own:
            copy.start()

    def middle():
        for copy, onward in zip(own[:2], relay):
            copy.wait_recv()
            onward.start()

    def end():
        for copy in own[2:] + relay:
            copy.wait_recv()
        for copy in own + relay:
            copy.wait_send()

    return begin, middle, end


def ring_sums(c, nc, rows, pbuf, sbuf, far_r, far_l, near_r, near_l, send, recv):
    right, left = shifted(c, 1, nc), shifted(c, -1, nc)
    opposite = shifted(c, 2, nc)
    half = rows // 2

    def at(block, part=None):
        if part is None:
            return aligned(block * rows, rows)
        return aligned(block * rows + part * half, half)

    def far(k):
        return (remote(sbuf.at[k, at(opposite, 0)], far_r.at[k], send.at[0, k], recv.at[0, k], ch=right),
                remote(sbuf.at[k, at(opposite, 1)], far_l.at[k], send.at[1, k], recv.at[1, k], ch=left))

    def near(k):
        return (remote(sbuf.at[k, at(right)], near_r.at[k], send.at[2, k], recv.at[2, k], ch=right),
                remote(sbuf.at[k, at(left)], near_l.at[k], send.at[3, k], recv.at[3, k], ch=left))

    def first(k, partial):
        pbuf[k] = partial
        sbuf[k] = partial.astype(BF16)
        for copy in far(k):
            copy.start()

    def second(k):
        to_right, to_left = far(k)
        onward = near(k)
        to_right.wait_recv()
        sbuf[k, at(right, 0)] = (pbuf[k, at(right, 0)] + far_r[k].astype(F32)).astype(BF16)
        onward[0].start()
        to_left.wait_recv()
        sbuf[k, at(left, 1)] = (pbuf[k, at(left, 1)] + far_l[k].astype(F32)).astype(BF16)
        onward[1].start()

    def third(k):
        for copy in near(k):
            copy.wait_recv()
        return pbuf[k, at(c)] + near_r[k].astype(F32) + near_l[k].astype(F32)

    def drain(k):
        for copy in far(k) + near(k):
            copy.wait_send()

    return first, second, third, drain


def layer_kernel(nw, nc, x_ref, seg_ref, wx, wy, wo, wg, wu, wd, gt_ref, bo_ref, gm_ref, bd_ref, bx_ref, by_ref, cb_ref, rb_ref, ib_ref, lam_ref, cw_ref, rg_ref, ig_ref, bg_ref, bu_ref,
                 out_ref, wx_all, wy_all, wo_all, wg_all, wu_all, wd_all,
                 xbuf, pbufs, pv_ref, pos_ref, wide_ref, xown, pars, nall, mall, wtile, ctile, stage_r, stage_c, ubuf, hsend, hrecv, ybuf, abuf, bbuf, tot, mixed, gbuf, inner, res,
                 pbuf, sbuf, far_r, far_l, near_r, near_l, osend, fin,
                 lsem, tsem, csem, outsem, xs, xr, ps, pr, ns, nr, hs, hr, ts, tr, as_, ar, ms, mr, ds, dr, os_, or_, fs, fr, ss, rs, ws, wr):
    w, c = lax.axis_index('wd'), lax.axis_index('ch')
    nx = nw // 2
    chip, core = w // 2, w % 2
    rows, part = xown.shape[0], xbuf.shape[2]
    tokens, chans = ybuf.shape
    width = part * nw

    def member(step, other):
        return shifted(chip, step, nx) * 2 + (core + other) % 2

    right_w, left_w, far_w, mate = member(1, 0), member(-1, 0), member(2, 0), member(0, 1)

    barrier = pltpu.get_barrier_semaphore()
    for d in range(1, nw):
        pl.semaphore_signal(barrier, inc=1, device_id={'wd': shifted(w, d, nw)}, device_id_type=MESH)
    for d in (1, -1):
        pl.semaphore_signal(barrier, inc=1, device_id={'ch': shifted(c, d, nc)}, device_id_type=MESH)
    pl.semaphore_wait(barrier, nw + 1)

    weights = ((wx, wx_all), (wy, wy_all), (wo, wo_all), (wg, wg_all), (wu, wu_all), (wd, wd_all))

    def stream(i):
        src, dst = weights[i]
        depth = src.shape[0]
        half = depth // 2

        def piece(block, k):
            return dst.at[aligned(block * depth + k * half, half)]

        low, high = src.at[pl.ds(0, half)], src.at[pl.ds(half, half)]
        mine = dst.at[aligned(w * depth, depth)]
        first_sends = ((low, piece(w, 0), right_w), (high, piece(w, 1), left_w), (high, piece(w, 1), right_w), (low, piece(w, 0), left_w), (src, mine, mate))
        relays = ((left_w, 0, right_w), (right_w, 1, left_w), (left_w, 0, mate), (right_w, 1, mate), (left_w, 1, mate), (right_w, 0, mate), (far_w, 0, mate), (far_w, 1, mate))

        def copy(k):
            if k < len(first_sends):
                source, target, to = first_sends[k]
            else:
                block, p, to = relays[k - len(first_sends)]
                source = target = piece(block, p)
            return remote(source, target, ss.at[i, k], rs.at[i, k], wd=to)

        if depth == part:
            stage = stage_r.at[:, pl.ds(0, src.shape[1])]
        else:
            stage = stage_c.at[pl.ds(0, depth)]

        def load():
            return pltpu.make_async_copy(src, stage, lsem.at[0])

        def keep():
            return pltpu.make_async_copy(stage, mine, lsem.at[1])

        def part_copy(kind, t):
            block, p, to = relays[(0, 1, 6, 7)[kind]]
            size = half // PIECES
            rows_of_piece = dst.at[aligned(block * depth + p * half + t * size, size)]
            return remote(rows_of_piece, rows_of_piece, ws.at[kind, t], wr.at[kind, t], wd=to)

        return copy, load, keep, part_copy

    def send_own(i):
        copy, load, keep, part_copy = stream(i)
        for k in range(5):
            copy(k).start()
        load().start()
        load().wait()
        keep().start()

    def send_on(i):
        copy, load, keep, part_copy = stream(i)
        last = i + 1 == len(weights)
        if not last:
            keep().wait()
        for k in range(2):
            copy(k).wait_recv()
            if last:
                for t in range(PIECES - 1):
                    part_copy(k, t).start()
            else:
                copy(5 + k).start()
            copy(7 + k).start()

    def send_on_and_next(i):
        send_on(i)
        send_own(i + 1)

    def ready(i):
        copy = stream(i)[0]
        for k, onward in ((2, 9), (3, 10), (5, 11), (6, 12)):
            copy(k).wait_recv()
            copy(onward).start()
        for k in (4, 7, 8, 9, 10, 11, 12):
            copy(k).wait_recv()

    def column_tiles(src, body):
        size = wtile.shape[2]
        count = src.shape[1] // size

        def load(j, slot):
            return pltpu.make_async_copy(src.at[:, aligned(j * size, size)], wtile.at[slot], tsem.at[slot])

        load(0, 0).start()

        def step(j, carry):
            slot = lax.rem(j, 2)

            @pl.when(j + 1 < count)
            def _():
                load(j + 1, 1 - slot).start()

            load(j, slot).wait()
            body(aligned(j * size, size), wtile[slot])
            return carry

        lax.fori_loop(0, count, step, 0)

    def rows_of(t):
        return x_ref.at[aligned((t * nc + c) * rows, rows)]

    def wide_row(ref):
        return ref[...].astype(F32)[None, :]

    for k, ref in enumerate((gt_ref, bo_ref, gm_ref, bd_ref)):
        pbufs[w, k:k + 1, :] = wide_row(ref)
    pbufs[w, 4:, :] = jnp.zeros((4, part), F32)
    own = pltpu.make_async_copy(rows_of(w), xbuf.at[w], lsem.at[2])
    own.start()
    copies = []
    for d in range(1, nw):
        t = shifted(w, d, nw)
        copies.append(remote(rows_of(t), xbuf.at[w], xs.at[d], xr.at[d], wd=t))
        copies.append(remote(pbufs.at[w], pbufs.at[w], ps.at[d], pr.at[d], wd=t))
    for copy in copies:
        copy.start()
    send_own(0)
    for k, ref in enumerate((bx_ref, by_ref, cb_ref, rb_ref, ib_ref)):
        pv_ref[k:k + 1, :] = wide_row(ref)
    lam = lam_ref[...][None, :]
    pv_ref[5:6, :] = -8.0 * (jnp.maximum(-lam, 0.0) + jnp.log1p(jnp.exp(-jnp.abs(lam))))
    pv_ref[6:10, :] = cw_ref[...].astype(F32)
    wide_ref[0:1, :] = wide_row(bg_ref)
    wide_ref[1:2, :] = wide_row(bu_ref)
    pos_row = seg_ref[0:1, aligned(w * tokens, tokens)].astype(F32)
    pos_cols = jnp.broadcast_to(pos_row, (128, tokens)).T.astype(jnp.int32)
    for k in range(pos_ref.shape[1] // 128):
        pos_ref[:, k * 128:(k + 1) * 128] = pos_cols
    own.wait()
    for copy in copies:
        copy.wait_recv()
    total = jnp.zeros((rows, 1), F32)
    for j in range(nw):
        vals = xbuf[j].astype(F32)
        total = total + jnp.sum(vals * vals, axis=1, keepdims=True)
    my_rows = aligned(c * rows, rows)
    for j in range(nw):
        cols = slice(j * part, (j + 1) * part)
        xown[:, cols] = xbuf[j]
        pars[:, cols] = pbufs[j]
        nall[my_rows, cols] = rms(xbuf[j].astype(F32), total, width, pbufs[j, 0:1])
    begin, middle, end = ring_gather(nall, c, nc, rows, ns, nr)
    begin()
    for copy in copies:
        copy.wait_send()
    send_on_and_next(0)
    middle()
    end()

    ready(0)

    def u_tile(cols, weight):
        u = jnp.dot(nall[...], weight, preferred_element_type=F32) + pv_ref[0:1, cols]
        ubuf[pl.ds(HALO, tokens), cols] = u.astype(BF16).astype(F32)

    column_tiles(wx_all, u_tile)
    hsend[...] = ubuf[pl.ds(tokens, HALO), :].astype(BF16)
    halo = remote(hsend, hrecv, hs.at[0], hr.at[0], wd=shifted(w, 1, nw))
    halo.start()
    send_on_and_next(1)
    ready(1)

    def y_tile(cols, weight):
        y = jnp.dot(nall[...], weight, preferred_element_type=F32) + pv_ref[1:2, cols]
        ybuf[:, cols] = jax.nn.gelu(y, approximate=True).astype(BF16)

    column_tiles(wy_all, y_tile)
    halo.wait()
    ubuf[pl.ds(0, HALO), :] = hrecv[...].astype(F32)
    blocks, bw = rg_ref.shape[0], rg_ref.shape[1]

    def gate_block(j, carry):
        cols = aligned(j * bw, bw)
        pos = pos_ref[...]
        conv = pv_ref[2:3, cols] + ubuf[pl.ds(HALO, tokens), cols] * pv_ref[6:7, cols]
        for k in range(1, 4):
            conv = conv + jnp.where(pos >= k, ubuf[pl.ds(HALO - k, tokens), cols], 0.0) * pv_ref[6 + k:7 + k, cols]
        conv = conv.astype(BF16)
        rate = jax.nn.sigmoid(jnp.dot(conv, rg_ref[j], preferred_element_type=F32) + pv_ref[3:4, cols])
        inflow = jax.nn.sigmoid(jnp.dot(conv, ig_ref[j], preferred_element_type=F32) + pv_ref[4:5, cols])
        log_a = rate * pv_ref[5:6, cols]
        a = jnp.exp(log_a)
        z = 2.0 * log_a
        series = 1.0 + z * (1.0 / 8.0)
        for k in range(7, 1, -1):
            series = 1.0 + z * series * (1.0 / k)
        gap = jnp.maximum(jnp.where(z > -0.5, -z * series, 1.0 - a * a), 0.0)
        root = jnp.where(gap > 0.0, gap * lax.rsqrt(jnp.where(gap > 0.0, gap, 1.0)), 0.0)
        reset = pos == 0
        abuf[:, cols] = jnp.where(reset, 0.0, a)
        bbuf[:, cols] = jnp.where(reset, 1.0, root) * inflow * conv.astype(F32)
        return carry

    lax.fori_loop(0, blocks, gate_block, 0)
    send_on(2)

    sub = lax.broadcasted_iota(jnp.int32, (TILE, chans), 0)

    def scan_tile(i, carry):
        a_in, h_in = carry
        at = aligned(i * TILE, TILE)
        a, b = abuf[at, :], bbuf[at, :]
        for d in (1, 2, 4):
            keep = sub >= d
            b = b + a * jnp.where(keep, pltpu.roll(b, d, 0), 0.0)
            a = a * jnp.where(keep, pltpu.roll(a, d, 0), 1.0)
        h = b + a * h_in
        a = a * a_in
        abuf[at, :] = a
        bbuf[at, :] = h
        return jnp.broadcast_to(a[TILE - 1:], a.shape), jnp.broadcast_to(h[TILE - 1:], h.shape)

    a_tot, h_tot = lax.fori_loop(0, tokens // TILE, scan_tile, (jnp.ones((TILE, chans), F32), jnp.zeros((TILE, chans), F32)))
    tot[w] = jnp.where(sub < TILE // 2, a_tot, h_tot)
    copies = []
    for d in range(1, nw):
        copies.append(remote(tot.at[w], tot.at[w], ts.at[d], tr.at[d], wd=shifted(w, d, nw)))
    for copy in copies:
        copy.start()
    send_own(3)
    for copy in copies:
        copy.wait_recv()
    h_in = jnp.zeros((1, chans), F32)
    for s in range(nw):
        h_in = jnp.where(s < w, tot[s, 0:1] * h_in + tot[s, TILE - 1:], h_in)
    for j in range(blocks):
        cols = slice(j * bw, (j + 1) * bw)
        hidden = bbuf[:, cols] + abuf[:, cols] * h_in[:, cols]
        mixed[:, cols] = (hidden * ybuf[:, cols].astype(F32)).astype(BF16)
    for copy in copies:
        copy.wait_send()

    ready(2)
    first, second, third, drain = ring_sums(c, nc, rows, pbuf, sbuf, far_r, far_l, near_r, near_l, as_, ar)

    def o_load(j, slot):
        return pltpu.make_async_copy(wo_all.at[aligned(j * chans, chans)], ctile.at[slot, pl.ds(0, chans)], csem.at[slot])

    o_load(0, 0).start()

    def o_step(k, carry):
        slot = lax.rem(k, 2)

        @pl.when(k + 1 < nw)
        def _():
            o_load(k + 1, 1 - slot).start()

        o_load(k, slot).wait()
        first(k, jnp.dot(mixed[...], ctile[slot, pl.ds(0, chans), :], preferred_element_type=F32))
        return carry

    def o_second(k, carry):
        second(k)
        return carry

    lax.fori_loop(0, nw, o_step, 0)
    lax.fori_loop(0, nw, o_second, 0)
    send_on_and_next(3)
    total = jnp.zeros((rows, 1), F32)
    for k in range(nw):
        cols = slice(k * part, (k + 1) * part)
        vals = xown[:, cols].astype(F32) + third(k) + pars[1:2, cols]
        res[:, cols] = vals
        total = total + jnp.sum(vals * vals, axis=1, keepdims=True)
    for k in range(nw):
        cols = slice(k * part, (k + 1) * part)
        mall[my_rows, cols] = rms(res[:, cols], total, width, pars[2:3, cols])
    begin, middle, end = ring_gather(mall, c, nc, rows, ms, mr)
    begin()

    def o_drain(k, carry):
        drain(k)
        return carry

    lax.fori_loop(0, nw, o_drain, 0)
    middle()
    end()

    ready(3)

    def g_tile(cols, weight):
        g = jnp.dot(mall[...], weight, preferred_element_type=F32) + wide_ref[0:1, cols]
        gbuf[:, cols] = jax.nn.gelu(g, approximate=True)

    column_tiles(wg_all, g_tile)
    send_on_and_next(4)
    ready(4)

    def i_tile(cols, weight):
        u = jnp.dot(mall[...], weight, preferred_element_type=F32) + wide_ref[1:2, cols]
        inner[:, cols] = (gbuf[:, cols] * u).astype(BF16)

    column_tiles(wu_all, i_tile)

    first, second, third, drain = ring_sums(c, nc, rows, pbuf, sbuf, far_r, far_l, near_r, near_l, ds, dr)
    right, left = shifted(c, 1, nc), shifted(c, -1, nc)
    half = rows // 2
    depth = wd.shape[0]

    targets = [member(step, other) for step, other in HOPS]
    sources = [member(-step, other) for step, other in HOPS]

    def block_of(d):
        return targets[d]

    def source_of(d):
        return sources[d]

    down, _, keep, part_copy = stream(5)

    def rows_at(owner, group, at=0, size=rows):
        return aligned((owner * nc + group) * rows + at, size)

    def hop(d):
        return remote(osend.at[d], fin.at[rows_at(w, c)], os_.at[d], or_.at[d], wd=block_of(d))

    def spread(d):
        piece = fin.at[rows_at(source_of(d), c)]
        return (remote(piece, piece, fs.at[0, d], fr.at[0, d], ch=right), remote(piece, piece, fs.at[1, d], fr.at[1, d], ch=left))

    def relay(d):
        from_left = fin.at[rows_at(source_of(d), left, 0, half)]
        from_right = fin.at[rows_at(source_of(d), right, half, half)]
        return (remote(from_left, from_left, fs.at[2, d], fr.at[2, d], ch=right), remote(from_right, from_right, fs.at[3, d], fr.at[3, d], ch=left))

    def finish(e):
        cols = aligned(block_of(e) * part, part)
        done = (res[:, cols] + third(e) + pars[3:4, cols]).astype(BF16)

        if e == 0:
            fin[rows_at(w, c), :] = done
        else:
            osend[e] = done
            hop(e).start()

    def share(e):
        if e > 0:
            hop(e).wait_recv()
        for copy in spread(e):
            copy.start()

    def pass_on(e):
        for copy, onward in zip(spread(e), relay(e)):
            copy.wait_recv()
            onward.start()

    def store(e):
        at = aligned(source_of(e) * tokens, tokens)
        return pltpu.make_async_copy(fin.at[at], out_ref.at[at], outsem.at[e])

    def complete(e):
        for copy in relay(e):
            copy.wait_recv()
        store(e).start()

    def fetch(d):
        return pltpu.make_async_copy(wd_all.at[aligned(block_of(d) * depth, depth)], ctile.at[d % 2], csem.at[d % 2])

    def multiply(d):
        fetch(d).wait()
        first(d, jnp.dot(inner[...], ctile[d % 2], preferred_element_type=F32))

    def take(*indices):
        for k in indices:
            down(k).wait_recv()

    def relay_piece(t):
        for k in range(2):
            part_copy(k, t).wait_recv()
            part_copy(2 + k, t).start()

    keep().wait()
    fetch(0).start()
    take(4)
    fetch(1).start()
    multiply(0)
    multiply(1)
    send_on(5)
    second(0)
    second(1)
    finish(0)
    share(0)
    finish(1)
    share(1)
    pass_on(0)
    pass_on(1)
    take(2, 3)
    fetch(2).start()
    fetch(3).start()
    down(9).start()
    down(10).start()
    multiply(2)
    take(7, 9)
    fetch(4).start()
    multiply(3)
    second(2)
    take(8, 10)
    fetch(5).start()
    multiply(4)
    second(3)
    finish(2)
    multiply(5)
    finish(3)
    for k in range(2):
        part_copy(k, PIECES - 1).start()
    second(4)
    for t in range(PIECES - 1):
        relay_piece(t)
    finish(4)
    second(5)
    finish(5)
    share(2)
    share(3)
    relay_piece(PIECES - 1)
    fetch(6).start()
    pass_on(2)
    pass_on(3)
    multiply(6)
    for t in range(PIECES):
        for k in range(2):
            part_copy(2 + k, t).wait_recv()
    fetch(7).start()
    share(4)
    share(5)
    multiply(7)
    second(6)
    pass_on(4)
    pass_on(5)
    second(7)
    finish(6)
    finish(7)
    share(6)
    share(7)
    for e in range(6):
        complete(e)
    pass_on(6)
    pass_on(7)
    complete(6)
    complete(7)
    for e in range(nw):
        for copy in spread(e) + relay(e):
            copy.wait_send()
        drain(e)
        if e > 0:
            hop(e).wait_send()
    for i in range(len(weights)):
        copy, _, _, part_copy = stream(i)
        last = i + 1 == len(weights)
        for k in range(13):
            if not (last and k in (5, 6, 11, 12)):
                copy(k).wait_send()
        if last:
            for kind in range(4):
                for t in range(PIECES):
                    part_copy(kind, t).wait_send()
    for k in range(nw):
        store(k).wait()


def dma(*shape):
    return pltpu.SemaphoreType.DMA(shape)


def solution(mesh):
    nw = mesh.shape['wd']
    nc = mesh.shape['ch']
    assert nc == 4 and nw == len(HOPS)
    row_spec = P('dp', 'wd')
    specs = (row_spec, P('dp', None), P('wd'), P('wd', 'ch'), P('ch'), P('wd', 'ch'), P('ch'), P(None, 'ch'), P('ch'), P('ch'), P('ch', None, None), P('ch'), P('ch', None, None), P('ch'), P('ch', 'wd'), P('wd'), P('wd'), P('wd', 'ch'), P('ch'), P('wd', 'ch'), P('ch'), P('ch', 'wd'), P('wd'))
    vm = pl.BlockSpec(memory_space=VMEM)
    anywhere = pl.BlockSpec(memory_space=ANY)

    def local_layer(resid_in, seg_pos, gain_temporal, w_x, bias_x, w_y, bias_y, conv_w, conv_bias, lam_param, rgate_w, rgate_b, igate_w, igate_b, w_o, bias_o, gain_mlp, w_g, bias_g, w_u, bias_u, w_d, bias_d):
        tokens, part = resid_in.shape
        width = part * nw
        span = tokens // nw
        rows = span // nc
        chans = w_x.shape[1]
        wide = w_g.shape[1]
        bw = rgate_w.shape[1]
        assert seg_pos.shape[0] == 1

        def landing(arr):
            return jax.ShapeDtypeStruct((arr.shape[0] * nw, arr.shape[1]), arr.dtype)

        stream = (w_x, w_y, w_o, w_g, w_u, w_d)
        scratch = [
            VMEM((nw, rows, part), BF16), VMEM((nw, 8, part), F32), VMEM((16, chans), F32), VMEM((span, bw), jnp.int32), VMEM((8, wide), F32), VMEM((rows, width), BF16), VMEM((8, width), F32),
            VMEM((span, width), BF16), VMEM((span, width), BF16), VMEM((2, width, bw), BF16), VMEM((2, wide, part), BF16),
            VMEM((part, wide), BF16), VMEM((wide, part), BF16),
            VMEM((span + HALO, chans), F32), VMEM((HALO, chans), BF16), VMEM((HALO, chans), BF16), VMEM((span, chans), BF16),
            VMEM((span, chans), F32), VMEM((span, chans), F32), VMEM((nw, TILE, chans), F32), VMEM((span, chans), BF16),
            VMEM((span, wide), F32), VMEM((span, wide), BF16), VMEM((rows, width), F32),
            VMEM((nw, span, part), F32), VMEM((nw, span, part), BF16), VMEM((nw, rows // 2, part), BF16), VMEM((nw, rows // 2, part), BF16),
            VMEM((nw, rows, part), BF16), VMEM((nw, rows, part), BF16), VMEM((nw, rows, part), BF16), VMEM((tokens, part), BF16),
            dma(4), dma(2), dma(2), dma(nw), dma(nw), dma(nw), dma(nw), dma(nw), dma(6), dma(6), dma(1), dma(1), dma(nw), dma(nw),
            dma(4, nw), dma(4, nw), dma(6), dma(6), dma(4, nw), dma(4, nw), dma(nw), dma(nw), dma(4, nw), dma(4, nw),
            dma(len(stream), 13), dma(len(stream), 13), dma(4, PIECES), dma(4, PIECES),
        ]
        return pl.pallas_call(
            functools.partial(layer_kernel, nw, nc), name='layer',
            out_shape=(jax.ShapeDtypeStruct((tokens, part), BF16),) + tuple(landing(arr) for arr in stream),
            in_specs=[anywhere] + [vm] + [anywhere] * 6 + [vm] * 15, out_specs=(anywhere,) * 7, scratch_shapes=scratch,
            compiler_params=pltpu.CompilerParams(vmem_limit_bytes=VMEM_LIMIT, collective_id=0, has_side_effects=True),
        )(resid_in, seg_pos, *stream, gain_temporal, bias_o, gain_mlp, bias_d, bias_x, bias_y, conv_bias, rgate_b, igate_b, lam_param, conv_w, rgate_w, igate_w, bias_g, bias_u)[0]

    return jax.shard_map(local_layer, mesh=mesh, in_specs=specs, out_specs=row_spec, check_vma=False)
```

```python
import functools

import jax
import jax.numpy as jnp
from jax import lax
from jax.experimental import pallas as pl
from jax.experimental.pallas import tpu as pltpu
from jax.sharding import PartitionSpec as P

EPS = 1e-6
PIECES = 3
F32 = jnp.float32
BF16 = jnp.bfloat16
MESH = pl.DeviceIdType.MESH
VMEM = pltpu.VMEM
ANY = pl.ANY
HALO = 16
TILE = 8
VMEM_LIMIT = 62 * 1024 * 1024
HOPS = ((0, 0), (0, 1), (-1, 0), (1, 0), (-1, 1), (1, 1), (2, 0), (2, 1))


def remote(src, dst, send, recv, **to):
    return pltpu.make_async_remote_copy(src_ref=src, dst_ref=dst, send_sem=send, recv_sem=recv, device_id=to, device_id_type=MESH)


def shifted(index, by, count):
    return lax.rem(index + (by % count), count)


def rms(vals, sum_sq, width, gain):
    return (vals * lax.rsqrt(sum_sq / width + EPS) * (1.0 + gain)).astype(BF16)


def aligned(start, size):
    return pl.ds(pl.multiple_of(start, size), size)


def ring_gather(buf, c, nc, rows, send, recv):
    right, left = shifted(c, 1, nc), shifted(c, -1, nc)
    half = rows // 2

    def make(block, part, to, k):
        piece = buf.at[aligned(block * rows + part * half, half)]
        return remote(piece, piece, send.at[k], recv.at[k], ch=to)

    own = [make(c, 0, right, 0), make(c, 1, left, 1), make(c, 1, right, 2), make(c, 0, left, 3)]
    relay = [make(left, 0, right, 4), make(right, 1, left, 5)]

    def begin():
        for copy in own:
            copy.start()

    def middle():
        for copy, onward in zip(own[:2], relay):
            copy.wait_recv()
            onward.start()

    def end():
        for copy in own[2:] + relay:
            copy.wait_recv()
        for copy in own + relay:
            copy.wait_send()

    return begin, middle, end


def ring_sums(c, nc, rows, pbuf, sbuf, far_r, far_l, near_r, near_l, send, recv):
    right, left = shifted(c, 1, nc), shifted(c, -1, nc)
    opposite = shifted(c, 2, nc)
    half = rows // 2

    def at(block, part=None):
        if part is None:
            return aligned(block * rows, rows)
        return aligned(block * rows + part * half, half)

    def far(k):
        return (remote(sbuf.at[k, at(opposite, 0)], far_r.at[k], send.at[0, k], recv.at[0, k], ch=right),
                remote(sbuf.at[k, at(opposite, 1)], far_l.at[k], send.at[1, k], recv.at[1, k], ch=left))

    def near(k):
        return (remote(sbuf.at[k, at(right)], near_r.at[k], send.at[2, k], recv.at[2, k], ch=right),
                remote(sbuf.at[k, at(left)], near_l.at[k], send.at[3, k], recv.at[3, k], ch=left))

    def first(k, partial):
        pbuf[k] = partial
        sbuf[k] = partial.astype(BF16)
        for copy in far(k):
            copy.start()

    def second(k):
        to_right, to_left = far(k)
        onward = near(k)
        to_right.wait_recv()
        sbuf[k, at(right, 0)] = (pbuf[k, at(right, 0)] + far_r[k].astype(F32)).astype(BF16)
        onward[0].start()
        to_left.wait_recv()
        sbuf[k, at(left, 1)] = (pbuf[k, at(left, 1)] + far_l[k].astype(F32)).astype(BF16)
        onward[1].start()

    def third(k):
        for copy in near(k):
            copy.wait_recv()
        return pbuf[k, at(c)] + near_r[k].astype(F32) + near_l[k].astype(F32)

    def drain(k):
        for copy in far(k) + near(k):
            copy.wait_send()

    return first, second, third, drain


def layer_kernel(nw, nc, x_ref, seg_ref, wx, wy, wo, wg, wu, wd, gt_ref, bo_ref, gm_ref, bd_ref, bx_ref, by_ref, cb_ref, rb_ref, ib_ref, lam_ref, cw_ref, rg_ref, ig_ref, bg_ref, bu_ref,
                 out_ref, wx_all, wy_all, wo_all, wg_all, wu_all, wd_all,
                 xbuf, pbufs, pv_ref, pos_ref, wide_ref, xown, pars, nall, mall, wtile, ctile, stage_r, stage_c, ubuf, hsend, hrecv, ybuf, abuf, bbuf, tot, mixed, gbuf, inner, res,
                 pbuf, sbuf, far_r, far_l, near_r, near_l, osend, fin,
                 lsem, tsem, csem, outsem, xs, xr, ps, pr, ns, nr, hs, hr, ts, tr, as_, ar, ms, mr, ds, dr, os_, or_, fs, fr, ss, rs, ws, wr):
    w, c = lax.axis_index('wd'), lax.axis_index('ch')
    nx = nw // 2
    chip, core = w // 2, w % 2
    rows, part = xown.shape[0], xbuf.shape[2]
    tokens, chans = ybuf.shape
    width = part * nw

    def member(step, other):
        return shifted(chip, step, nx) * 2 + (core + other) % 2

    right_w, left_w, far_w, mate = member(1, 0), member(-1, 0), member(2, 0), member(0, 1)

    barrier = pltpu.get_barrier_semaphore()
    for d in range(1, nw):
        pl.semaphore_signal(barrier, inc=1, device_id={'wd': shifted(w, d, nw)}, device_id_type=MESH)
    for d in (1, -1):
        pl.semaphore_signal(barrier, inc=1, device_id={'ch': shifted(c, d, nc)}, device_id_type=MESH)
    pl.semaphore_wait(barrier, nw + 1)

    weights = ((wx, wx_all), (wy, wy_all), (wo, wo_all), (wg, wg_all), (wu, wu_all), (wd, wd_all))

    def stream(i):
        src, dst = weights[i]
        depth = src.shape[0]
        half = depth // 2

        def piece(block, k):
            return dst.at[aligned(block * depth + k * half, half)]

        low, high = src.at[pl.ds(0, half)], src.at[pl.ds(half, half)]
        mine = dst.at[aligned(w * depth, depth)]
        first_sends = ((low, piece(w, 0), right_w), (high, piece(w, 1), left_w), (high, piece(w, 1), right_w), (low, piece(w, 0), left_w), (src, mine, mate))
        relays = ((left_w, 0, right_w), (right_w, 1, left_w), (left_w, 0, mate), (right_w, 1, mate), (left_w, 1, mate), (right_w, 0, mate), (far_w, 0, mate), (far_w, 1, mate))

        def copy(k):
            if k < len(first_sends):
                source, target, to = first_sends[k]
            else:
                block, p, to = relays[k - len(first_sends)]
                source = target = piece(block, p)
            return remote(source, target, ss.at[i, k], rs.at[i, k], wd=to)

        if depth == part:
            stage = stage_r.at[:, pl.ds(0, src.shape[1])]
        else:
            stage = stage_c.at[pl.ds(0, depth)]

        def load():
            return pltpu.make_async_copy(src, stage, lsem.at[0])

        def keep():
            return pltpu.make_async_copy(stage, mine, lsem.at[1])

        def part_copy(kind, t):
            block, p, to = relays[(0, 1, 6, 7)[kind]]
            size = half // PIECES
            rows_of_piece = dst.at[aligned(block * depth + p * half + t * size, size)]
            return remote(rows_of_piece, rows_of_piece, ws.at[kind, t], wr.at[kind, t], wd=to)

        return copy, load, keep, part_copy

    def send_own(i):
        copy, load, keep, part_copy = stream(i)
        for k in range(5):
            copy(k).start()
        load().start()
        load().wait()
        keep().start()

    def send_on(i):
        copy, load, keep, part_copy = stream(i)
        last = i + 1 == len(weights)
        if not last:
            keep().wait()
        for k in range(2):
            copy(k).wait_recv()
            if last:
                for t in range(PIECES - 1):
                    part_copy(k, t).start()
            else:
                copy(5 + k).start()
            copy(7 + k).start()

    def send_on_and_next(i):
        send_on(i)
        send_own(i + 1)

    def ready(i):
        copy = stream(i)[0]
        for k, onward in ((2, 9), (3, 10), (5, 11), (6, 12)):
            copy(k).wait_recv()
            copy(onward).start()
        for k in (4, 7, 8, 9, 10, 11, 12):
            copy(k).wait_recv()

    def column_tiles(src, body):
        size = wtile.shape[2]
        count = src.shape[1] // size

        def load(j, slot):
            return pltpu.make_async_copy(src.at[:, aligned(j * size, size)], wtile.at[slot], tsem.at[slot])

        load(0, 0).start()

        def step(j, carry):
            slot = lax.rem(j, 2)

            @pl.when(j + 1 < count)
            def _():
                load(j + 1, 1 - slot).start()

            load(j, slot).wait()
            body(aligned(j * size, size), wtile[slot])
            return carry

        lax.fori_loop(0, count, step, 0)

    def rows_of(t):
        return x_ref.at[aligned((t * nc + c) * rows, rows)]

    def wide_row(ref):
        return ref[...].astype(F32)[None, :]

    for k, ref in enumerate((gt_ref, bo_ref, gm_ref, bd_ref)):
        pbufs[w, k:k + 1, :] = wide_row(ref)
    pbufs[w, 4:, :] = jnp.zeros((4, part), F32)
    own = pltpu.make_async_copy(rows_of(w), xbuf.at[w], lsem.at[2])
    own.start()
    copies = []
    for d in range(1, nw):
        t = shifted(w, d, nw)
        copies.append(remote(rows_of(t), xbuf.at[w], xs.at[d], xr.at[d], wd=t))
        copies.append(remote(pbufs.at[w], pbufs.at[w], ps.at[d], pr.at[d], wd=t))
    for copy in copies:
        copy.start()
    send_own(0)
    for k, ref in enumerate((bx_ref, by_ref, cb_ref, rb_ref, ib_ref)):
        pv_ref[k:k + 1, :] = wide_row(ref)
    lam = lam_ref[...][None, :]
    pv_ref[5:6, :] = -8.0 * (jnp.maximum(-lam, 0.0) + jnp.log1p(jnp.exp(-jnp.abs(lam))))
    pv_ref[6:10, :] = cw_ref[...].astype(F32)
    wide_ref[0:1, :] = wide_row(bg_ref)
    wide_ref[1:2, :] = wide_row(bu_ref)
    pos_row = seg_ref[0:1, aligned(w * tokens, tokens)].astype(F32)
    pos_cols = jnp.broadcast_to(pos_row, (128, tokens)).T.astype(jnp.int32)
    for k in range(pos_ref.shape[1] // 128):
        pos_ref[:, k * 128:(k + 1) * 128] = pos_cols
    own.wait()
    for copy in copies:
        copy.wait_recv()
    total = jnp.zeros((rows, 1), F32)
    for j in range(nw):
        vals = xbuf[j].astype(F32)
        total = total + jnp.sum(vals * vals, axis=1, keepdims=True)
    my_rows = aligned(c * rows, rows)
    for j in range(nw):
        cols = slice(j * part, (j + 1) * part)
        xown[:, cols] = xbuf[j]
        pars[:, cols] = pbufs[j]
        nall[my_rows, cols] = rms(xbuf[j].astype(F32), total, width, pbufs[j, 0:1])
    begin, middle, end = ring_gather(nall, c, nc, rows, ns, nr)
    begin()
    for copy in copies:
        copy.wait_send()
    send_on_and_next(0)
    middle()
    end()

    ready(0)

    def u_tile(cols, weight):
        u = jnp.dot(nall[...], weight, preferred_element_type=F32) + pv_ref[0:1, cols]
        ubuf[pl.ds(HALO, tokens), cols] = u.astype(BF16).astype(F32)

    column_tiles(wx_all, u_tile)
    hsend[...] = ubuf[pl.ds(tokens, HALO), :].astype(BF16)
    halo = remote(hsend, hrecv, hs.at[0], hr.at[0], wd=shifted(w, 1, nw))
    halo.start()
    send_on_and_next(1)
    ready(1)

    def y_tile(cols, weight):
        y = jnp.dot(nall[...], weight, preferred_element_type=F32) + pv_ref[1:2, cols]
        ybuf[:, cols] = jax.nn.gelu(y, approximate=True).astype(BF16)

    column_tiles(wy_all, y_tile)
    halo.wait()
    ubuf[pl.ds(0, HALO), :] = hrecv[...].astype(F32)
    blocks, bw = rg_ref.shape[0], rg_ref.shape[1]

    def gate_block(j, carry):
        cols = aligned(j * bw, bw)
        pos = pos_ref[...]
        conv = pv_ref[2:3, cols] + ubuf[pl.ds(HALO, tokens), cols] * pv_ref[6:7, cols]
        for k in range(1, 4):
            conv = conv + jnp.where(pos >= k, ubuf[pl.ds(HALO - k, tokens), cols], 0.0) * pv_ref[6 + k:7 + k, cols]
        conv = conv.astype(BF16)
        rate = jax.nn.sigmoid(jnp.dot(conv, rg_ref[j], preferred_element_type=F32) + pv_ref[3:4, cols])
        inflow = jax.nn.sigmoid(jnp.dot(conv, ig_ref[j], preferred_element_type=F32) + pv_ref[4:5, cols])
        log_a = rate * pv_ref[5:6, cols]
        a = jnp.exp(log_a)
        z = 2.0 * log_a
        series = 1.0 + z * (1.0 / 8.0)
        for k in range(7, 1, -1):
            series = 1.0 + z * series * (1.0 / k)
        gap = jnp.maximum(jnp.where(z > -0.5, -z * series, 1.0 - a * a), 0.0)
        root = jnp.where(gap > 0.0, gap * lax.rsqrt(jnp.where(gap > 0.0, gap, 1.0)), 0.0)
        reset = pos == 0
        abuf[:, cols] = jnp.where(reset, 0.0, a)
        bbuf[:, cols] = jnp.where(reset, 1.0, root) * inflow * conv.astype(F32)
        return carry

    lax.fori_loop(0, blocks, gate_block, 0)
    send_on(2)

    sub = lax.broadcasted_iota(jnp.int32, (TILE, chans), 0)

    def scan_tile(i, carry):
        a_in, h_in = carry
        at = aligned(i * TILE, TILE)
        a, b = abuf[at, :], bbuf[at, :]
        for d in (1, 2, 4):
            keep = sub >= d
            b = b + a * jnp.where(keep, pltpu.roll(b, d, 0), 0.0)
            a = a * jnp.where(keep, pltpu.roll(a, d, 0), 1.0)
        h = b + a * h_in
        a = a * a_in
        abuf[at, :] = a
        bbuf[at, :] = h
        return jnp.broadcast_to(a[TILE - 1:], a.shape), jnp.broadcast_to(h[TILE - 1:], h.shape)

    a_tot, h_tot = lax.fori_loop(0, tokens // TILE, scan_tile, (jnp.ones((TILE, chans), F32), jnp.zeros((TILE, chans), F32)))
    tot[w] = jnp.where(sub < TILE // 2, a_tot, h_tot)
    copies = []
    for d in range(1, nw):
        copies.append(remote(tot.at[w], tot.at[w], ts.at[d], tr.at[d], wd=shifted(w, d, nw)))
    for copy in copies:
        copy.start()
    send_own(3)
    for copy in copies:
        copy.wait_recv()
    h_in = jnp.zeros((1, chans), F32)
    for s in range(nw):
        h_in = jnp.where(s < w, tot[s, 0:1] * h_in + tot[s, TILE - 1:], h_in)
    for j in range(blocks):
        cols = slice(j * bw, (j + 1) * bw)
        hidden = bbuf[:, cols] + abuf[:, cols] * h_in[:, cols]
        mixed[:, cols] = (hidden * ybuf[:, cols].astype(F32)).astype(BF16)
    for copy in copies:
        copy.wait_send()

    ready(2)
    first, second, third, drain = ring_sums(c, nc, rows, pbuf, sbuf, far_r, far_l, near_r, near_l, as_, ar)

    def o_load(j, slot):
        return pltpu.make_async_copy(wo_all.at[aligned(j * chans, chans)], ctile.at[slot, pl.ds(0, chans)], csem.at[slot])

    o_load(0, 0).start()

    def o_step(k, carry):
        slot = lax.rem(k, 2)

        @pl.when(k + 1 < nw)
        def _():
            o_load(k + 1, 1 - slot).start()

        o_load(k, slot).wait()
        first(k, jnp.dot(mixed[...], ctile[slot, pl.ds(0, chans), :], preferred_element_type=F32))
        return carry

    def o_second(k, carry):
        second(k)
        return carry

    lax.fori_loop(0, nw, o_step, 0)
    lax.fori_loop(0, nw, o_second, 0)
    send_on_and_next(3)
    total = jnp.zeros((rows, 1), F32)
    for k in range(nw):
        cols = slice(k * part, (k + 1) * part)
        vals = xown[:, cols].astype(F32) + third(k) + pars[1:2, cols]
        res[:, cols] = vals
        total = total + jnp.sum(vals * vals, axis=1, keepdims=True)
    for k in range(nw):
        cols = slice(k * part, (k + 1) * part)
        mall[my_rows, cols] = rms(res[:, cols], total, width, pars[2:3, cols])
    begin, middle, end = ring_gather(mall, c, nc, rows, ms, mr)
    begin()

    def o_drain(k, carry):
        drain(k)
        return carry

    lax.fori_loop(0, nw, o_drain, 0)
    middle()
    end()

    ready(3)

    def g_tile(cols, weight):
        g = jnp.dot(mall[...], weight, preferred_element_type=F32) + wide_ref[0:1, cols]
        gbuf[:, cols] = jax.nn.gelu(g, approximate=True)

    column_tiles(wg_all, g_tile)
    send_on_and_next(4)
    ready(4)

    def i_tile(cols, weight):
        u = jnp.dot(mall[...], weight, preferred_element_type=F32) + wide_ref[1:2, cols]
        inner[:, cols] = (gbuf[:, cols] * u).astype(BF16)

    column_tiles(wu_all, i_tile)

    first, second, third, drain = ring_sums(c, nc, rows, pbuf, sbuf, far_r, far_l, near_r, near_l, ds, dr)
    right, left = shifted(c, 1, nc), shifted(c, -1, nc)
    half = rows // 2
    depth = wd.shape[0]

    targets = [member(step, other) for step, other in HOPS]
    sources = [member(-step, other) for step, other in HOPS]

    def block_of(d):
        return targets[d]

    def source_of(d):
        return sources[d]

    down, _, keep, part_copy = stream(5)

    def rows_at(owner, group, at=0, size=rows):
        return aligned((owner * nc + group) * rows + at, size)

    def hop(d):
        return remote(osend.at[d], fin.at[rows_at(w, c)], os_.at[d], or_.at[d], wd=block_of(d))

    def spread(d):
        piece = fin.at[rows_at(source_of(d), c)]
        return (remote(piece, piece, fs.at[0, d], fr.at[0, d], ch=right), remote(piece, piece, fs.at[1, d], fr.at[1, d], ch=left))

    def relay(d):
        from_left = fin.at[rows_at(source_of(d), left, 0, half)]
        from_right = fin.at[rows_at(source_of(d), right, half, half)]
        return (remote(from_left, from_left, fs.at[2, d], fr.at[2, d], ch=right), remote(from_right, from_right, fs.at[3, d], fr.at[3, d], ch=left))

    def finish(e):
        cols = aligned(block_of(e) * part, part)
        done = (res[:, cols] + third(e) + pars[3:4, cols]).astype(BF16)

        if e == 0:
            fin[rows_at(w, c), :] = done
        else:
            osend[e] = done
            hop(e).start()

    def share(e):
        if e > 0:
            hop(e).wait_recv()
        for copy in spread(e):
            copy.start()

    def pass_on(e):
        for copy, onward in zip(spread(e), relay(e)):
            copy.wait_recv()
            onward.start()

    def store(e):
        at = aligned(source_of(e) * tokens, tokens)
        return pltpu.make_async_copy(fin.at[at], out_ref.at[at], outsem.at[e])

    def complete(e):
        for copy in relay(e):
            copy.wait_recv()
        store(e).start()

    def fetch(d):
        return pltpu.make_async_copy(wd_all.at[aligned(block_of(d) * depth, depth)], ctile.at[d % 2], csem.at[d % 2])

    def multiply(d):
        fetch(d).wait()
        first(d, jnp.dot(inner[...], ctile[d % 2], preferred_element_type=F32))

    def take(*indices):
        for k in indices:
            down(k).wait_recv()

    def relay_piece(t):
        for k in range(2):
            part_copy(k, t).wait_recv()
            part_copy(2 + k, t).start()

    keep().wait()
    fetch(0).start()
    take(4)
    fetch(1).start()
    multiply(0)
    multiply(1)
    send_on(5)
    second(0)
    second(1)
    finish(0)
    share(0)
    finish(1)
    share(1)
    pass_on(0)
    pass_on(1)
    take(2, 3)
    fetch(2).start()
    fetch(3).start()
    down(9).start()
    down(10).start()
    multiply(2)
    take(7, 9)
    fetch(4).start()
    multiply(3)
    second(2)
    take(8, 10)
    fetch(5).start()
    multiply(4)
    second(3)
    finish(2)
    multiply(5)
    finish(3)
    for k in range(2):
        part_copy(k, PIECES - 1).start()
    second(4)
    for t in range(PIECES - 1):
        relay_piece(t)
    second(5)
    share(2)
    finish(4)
    share(3)
    finish(5)
    relay_piece(PIECES - 1)
    fetch(6).start()
    pass_on(2)
    multiply(6)
    for t in range(PIECES):
        for k in range(2):
            part_copy(2 + k, t).wait_recv()
    fetch(7).start()
    share(4)
    multiply(7)
    pass_on(3)
    second(6)
    share(5)
    second(7)
    pass_on(4)
    finish(6)
    pass_on(5)
    finish(7)
    share(6)
    for e in range(4):
        complete(e)
    share(7)
    pass_on(6)
    complete(4)
    complete(5)
    pass_on(7)
    complete(6)
    complete(7)
    for e in range(nw):
        for copy in spread(e) + relay(e):
            copy.wait_send()
        drain(e)
        if e > 0:
            hop(e).wait_send()
    for i in range(len(weights)):
        copy, _, _, part_copy = stream(i)
        last = i + 1 == len(weights)
        for k in range(13):
            if not (last and k in (5, 6, 11, 12)):
                copy(k).wait_send()
        if last:
            for kind in range(4):
                for t in range(PIECES):
                    part_copy(kind, t).wait_send()
    for k in range(nw):
        store(k).wait()


def dma(*shape):
    return pltpu.SemaphoreType.DMA(shape)


def solution(mesh):
    nw = mesh.shape['wd']
    nc = mesh.shape['ch']
    assert nc == 4 and nw == len(HOPS)
    row_spec = P('dp', 'wd')
    specs = (row_spec, P('dp', None), P('wd'), P('wd', 'ch'), P('ch'), P('wd', 'ch'), P('ch'), P(None, 'ch'), P('ch'), P('ch'), P('ch', None, None), P('ch'), P('ch', None, None), P('ch'), P('ch', 'wd'), P('wd'), P('wd'), P('wd', 'ch'), P('ch'), P('wd', 'ch'), P('ch'), P('ch', 'wd'), P('wd'))
    vm = pl.BlockSpec(memory_space=VMEM)
    anywhere = pl.BlockSpec(memory_space=ANY)

    def local_layer(resid_in, seg_pos, gain_temporal, w_x, bias_x, w_y, bias_y, conv_w, conv_bias, lam_param, rgate_w, rgate_b, igate_w, igate_b, w_o, bias_o, gain_mlp, w_g, bias_g, w_u, bias_u, w_d, bias_d):
        tokens, part = resid_in.shape
        width = part * nw
        span = tokens // nw
        rows = span // nc
        chans = w_x.shape[1]
        wide = w_g.shape[1]
        bw = rgate_w.shape[1]
        assert seg_pos.shape[0] == 1

        def landing(arr):
            return jax.ShapeDtypeStruct((arr.shape[0] * nw, arr.shape[1]), arr.dtype)

        stream = (w_x, w_y, w_o, w_g, w_u, w_d)
        scratch = [
            VMEM((nw, rows, part), BF16), VMEM((nw, 8, part), F32), VMEM((16, chans), F32), VMEM((span, bw), jnp.int32), VMEM((8, wide), F32), VMEM((rows, width), BF16), VMEM((8, width), F32),
            VMEM((span, width), BF16), VMEM((span, width), BF16), VMEM((2, width, bw), BF16), VMEM((2, wide, part), BF16),
            VMEM((part, wide), BF16), VMEM((wide, part), BF16),
            VMEM((span + HALO, chans), F32), VMEM((HALO, chans), BF16), VMEM((HALO, chans), BF16), VMEM((span, chans), BF16),
            VMEM((span, chans), F32), VMEM((span, chans), F32), VMEM((nw, TILE, chans), F32), VMEM((span, chans), BF16),
            VMEM((span, wide), F32), VMEM((span, wide), BF16), VMEM((rows, width), F32),
            VMEM((nw, span, part), F32), VMEM((nw, span, part), BF16), VMEM((nw, rows // 2, part), BF16), VMEM((nw, rows // 2, part), BF16),
            VMEM((nw, rows, part), BF16), VMEM((nw, rows, part), BF16), VMEM((nw, rows, part), BF16), VMEM((tokens, part), BF16),
            dma(4), dma(2), dma(2), dma(nw), dma(nw), dma(nw), dma(nw), dma(nw), dma(6), dma(6), dma(1), dma(1), dma(nw), dma(nw),
            dma(4, nw), dma(4, nw), dma(6), dma(6), dma(4, nw), dma(4, nw), dma(nw), dma(nw), dma(4, nw), dma(4, nw),
            dma(len(stream), 13), dma(len(stream), 13), dma(4, PIECES), dma(4, PIECES),
        ]
        return pl.pallas_call(
            functools.partial(layer_kernel, nw, nc), name='layer',
            out_shape=(jax.ShapeDtypeStruct((tokens, part), BF16),) + tuple(landing(arr) for arr in stream),
            in_specs=[anywhere] + [vm] + [anywhere] * 6 + [vm] * 15, out_specs=(anywhere,) * 7, scratch_shapes=scratch,
            compiler_params=pltpu.CompilerParams(vmem_limit_bytes=VMEM_LIMIT, collective_id=0, has_side_effects=True),
        )(resid_in, seg_pos, *stream, gain_temporal, bias_o, gain_mlp, bias_d, bias_x, bias_y, conv_bias, rgate_b, igate_b, lam_param, conv_w, rgate_w, igate_w, bias_g, bias_u)[0]

    return jax.shard_map(local_layer, mesh=mesh, in_specs=specs, out_specs=row_spec, check_vma=False)
```

```python
import functools

import jax
import jax.numpy as jnp
from jax import lax
from jax.experimental import pallas as pl
from jax.experimental.pallas import tpu as pltpu
from jax.sharding import PartitionSpec as P

EPS = 1e-6
PIECES = 3
F32 = jnp.float32
BF16 = jnp.bfloat16
MESH = pl.DeviceIdType.MESH
VMEM = pltpu.VMEM
ANY = pl.ANY
HALO = 16
TILE = 8
VMEM_LIMIT = 62 * 1024 * 1024


def remote(src, dst, send, recv, **to):
    return pltpu.make_async_remote_copy(src_ref=src, dst_ref=dst, send_sem=send, recv_sem=recv, device_id=to, device_id_type=MESH)


def shifted(index, by, count):
    return lax.rem(index + (by % count), count)


def rms(vals, sum_sq, width, gain):
    return (vals * lax.rsqrt(sum_sq / width + EPS) * (1.0 + gain)).astype(BF16)


def aligned(start, size):
    return pl.ds(pl.multiple_of(start, size), size)


def ring_gather(buf, c, nc, rows, send, recv):
    right, left = shifted(c, 1, nc), shifted(c, -1, nc)
    half = rows // 2

    def make(block, part, to, k):
        piece = buf.at[aligned(block * rows + part * half, half)]
        return remote(piece, piece, send.at[k], recv.at[k], ch=to)

    own = [make(c, 0, right, 0), make(c, 1, left, 1), make(c, 1, right, 2), make(c, 0, left, 3)]
    relay = [make(left, 0, right, 4), make(right, 1, left, 5)]

    def begin():
        for copy in own:
            copy.start()

    def middle():
        for copy, onward in zip(own[:2], relay):
            copy.wait_recv()
            onward.start()

    def end():
        for copy in own[2:] + relay:
            copy.wait_recv()
        for copy in own + relay:
            copy.wait_send()

    return begin, middle, end


def ring_sums(c, nc, rows, pbuf, sbuf, far_r, far_l, near_r, near_l, send, recv):
    right, left = shifted(c, 1, nc), shifted(c, -1, nc)
    opposite = shifted(c, 2, nc)
    half = rows // 2

    def at(block, part=None):
        if part is None:
            return aligned(block * rows, rows)
        return aligned(block * rows + part * half, half)

    def far(k):
        return (remote(sbuf.at[k, at(opposite, 0)], far_r.at[k], send.at[0, k], recv.at[0, k], ch=right),
                remote(sbuf.at[k, at(opposite, 1)], far_l.at[k], send.at[1, k], recv.at[1, k], ch=left))

    def near(k):
        return (remote(sbuf.at[k, at(right)], near_r.at[k], send.at[2, k], recv.at[2, k], ch=right),
                remote(sbuf.at[k, at(left)], near_l.at[k], send.at[3, k], recv.at[3, k], ch=left))

    def first(k, partial):
        pbuf[k] = partial
        sbuf[k] = partial.astype(BF16)
        for copy in far(k):
            copy.start()

    def second(k):
        to_right, to_left = far(k)
        onward = near(k)
        to_right.wait_recv()
        sbuf[k, at(right, 0)] = (pbuf[k, at(right, 0)] + far_r[k].astype(F32)).astype(BF16)
        onward[0].start()
        to_left.wait_recv()
        sbuf[k, at(left, 1)] = (pbuf[k, at(left, 1)] + far_l[k].astype(F32)).astype(BF16)
        onward[1].start()

    def third(k):
        for copy in near(k):
            copy.wait_recv()
        return pbuf[k, at(c)] + near_r[k].astype(F32) + near_l[k].astype(F32)

    def drain(k):
        for copy in far(k) + near(k):
            copy.wait_send()

    return first, second, third, drain


def layer_kernel(nw, nc, x_ref, seg_ref, wx, wy, wo, wg, wu, wd, gt_ref, bo_ref, gm_ref, bd_ref, bx_ref, by_ref, cb_ref, rb_ref, ib_ref, lam_ref, cw_ref, rg_ref, ig_ref, bg_ref, bu_ref,
                 out_ref, wx_all, wy_all, wo_all, wg_all, wu_all, wd_all,
                 xbuf, pbufs, pv_ref, pos_ref, wide_ref, xown, pars, nall, mall, wtile, ctile, stage_r, stage_c, ubuf, hsend, hrecv, ybuf, abuf, bbuf, tot, mixed, gbuf, inner, res,
                 pbuf, sbuf, far_r, far_l, near_r, near_l, osend, fin,
                 lsem, tsem, csem, outsem, xs, xr, ps, pr, ns, nr, hs, hr, ts, tr, as_, ar, ms, mr, ds, dr, os_, or_, fs, fr, ss, rs, ws, wr):
    w, c = lax.axis_index('wd'), lax.axis_index('ch')
    nx = nw // 2
    chip, core = w // 2, w % 2
    rows, part = xown.shape[0], xbuf.shape[2]
    tokens, chans = ybuf.shape
    width = part * nw

    def member(step, other):
        return shifted(chip, step, nx) * 2 + (core + other) % 2

    lead = jnp.where(core == 0, 1, nx - 1)

    def beside(step, other):
        return lax.rem(chip + step, nx) * 2 + (core + other) % 2

    fore_w, back_w = beside(lead, 0), beside(nx - lead, 0)
    right_w, left_w, far_w, mate = member(1, 0), member(-1, 0), member(2, 0), member(0, 1)

    barrier = pltpu.get_barrier_semaphore()
    for d in range(1, nw):
        pl.semaphore_signal(barrier, inc=1, device_id={'wd': shifted(w, d, nw)}, device_id_type=MESH)
    for d in (1, -1):
        pl.semaphore_signal(barrier, inc=1, device_id={'ch': shifted(c, d, nc)}, device_id_type=MESH)
    pl.semaphore_wait(barrier, nw + 1)

    weights = ((wx, wx_all), (wy, wy_all), (wo, wo_all), (wg, wg_all), (wu, wu_all), (wd, wd_all))

    def stream(i):
        src, dst = weights[i]
        depth = src.shape[0]
        half = depth // 2

        def piece(block, k):
            return dst.at[aligned(block * depth + k * half, half)]

        low, high = src.at[pl.ds(0, half)], src.at[pl.ds(half, half)]
        mine = dst.at[aligned(w * depth, depth)]
        last = i + 1 == len(weights)
        if last:
            first_sends = ((low, piece(w, 0), fore_w), (high, piece(w, 1), fore_w), (high, piece(w, 1), back_w), (low, piece(w, 0), back_w), (src, mine, mate))
            relays = ((back_w, 0, fore_w), (fore_w, 1, back_w), (back_w, 0, mate), (back_w, 1, mate), (fore_w, 1, mate), (fore_w, 0, mate), (far_w, 0, mate), (far_w, 1, mate))
        else:
            first_sends = ((low, piece(w, 0), right_w), (high, piece(w, 1), left_w), (high, piece(w, 1), right_w), (low, piece(w, 0), left_w), (src, mine, mate))
            relays = ((left_w, 0, right_w), (right_w, 1, left_w), (left_w, 0, mate), (right_w, 1, mate), (left_w, 1, mate), (right_w, 0, mate), (far_w, 0, mate), (far_w, 1, mate))

        def copy(k):
            if k < len(first_sends):
                source, target, to = first_sends[k]
            else:
                block, p, to = relays[k - len(first_sends)]
                source = target = piece(block, p)
            return remote(source, target, ss.at[i, k], rs.at[i, k], wd=to)

        if depth == part:
            stage = stage_r.at[:, pl.ds(0, src.shape[1])]
        else:
            stage = stage_c.at[pl.ds(0, depth)]

        def load():
            return pltpu.make_async_copy(src, stage, lsem.at[0])

        def keep():
            return pltpu.make_async_copy(stage, mine, lsem.at[1])

        def part_copy(kind, t):
            block, p, to = relays[(0, 1, 6, 7)[kind]]
            size = half // PIECES
            rows_of_piece = dst.at[aligned(block * depth + p * half + t * size, size)]
            return remote(rows_of_piece, rows_of_piece, ws.at[kind, t], wr.at[kind, t], wd=to)

        return copy, load, keep, part_copy

    def send_own(i):
        copy, load, keep, part_copy = stream(i)
        for k in range(5):
            if i + 1 < len(weights) or k not in (2, 3):
                copy(k).start()
        load().start()
        load().wait()
        keep().start()

    def send_on(i):
        copy, load, keep, part_copy = stream(i)
        keep().wait()
        for k in range(2):
            copy(k).wait_recv()
            copy(5 + k).start()
            copy(7 + k).start()

    def send_on_and_next(i):
        send_on(i)
        send_own(i + 1)

    def ready(i):
        copy = stream(i)[0]
        for k, onward in ((2, 9), (3, 10), (5, 11), (6, 12)):
            copy(k).wait_recv()
            copy(onward).start()
        for k in (4, 7, 8, 9, 10, 11, 12):
            copy(k).wait_recv()

    def column_tiles(src, body):
        size = wtile.shape[2]
        count = src.shape[1] // size

        def load(j, slot):
            return pltpu.make_async_copy(src.at[:, aligned(j * size, size)], wtile.at[slot], tsem.at[slot])

        load(0, 0).start()

        def step(j, carry):
            slot = lax.rem(j, 2)

            @pl.when(j + 1 < count)
            def _():
                load(j + 1, 1 - slot).start()

            load(j, slot).wait()
            body(aligned(j * size, size), wtile[slot])
            return carry

        lax.fori_loop(0, count, step, 0)

    def rows_of(t):
        return x_ref.at[aligned((t * nc + c) * rows, rows)]

    def wide_row(ref):
        return ref[...].astype(F32)[None, :]

    for k, ref in enumerate((gt_ref, bo_ref, gm_ref, bd_ref)):
        pbufs[w, k:k + 1, :] = wide_row(ref)
    pbufs[w, 4:, :] = jnp.zeros((4, part), F32)
    own = pltpu.make_async_copy(rows_of(w), xbuf.at[w], lsem.at[2])
    own.start()
    copies = []
    for d in range(1, nw):
        t = shifted(w, d, nw)
        copies.append(remote(rows_of(t), xbuf.at[w], xs.at[d], xr.at[d], wd=t))
        copies.append(remote(pbufs.at[w], pbufs.at[w], ps.at[d], pr.at[d], wd=t))
    for copy in copies:
        copy.start()
    send_own(0)
    for k, ref in enumerate((bx_ref, by_ref, cb_ref, rb_ref, ib_ref)):
        pv_ref[k:k + 1, :] = wide_row(ref)
    lam = lam_ref[...][None, :]
    pv_ref[5:6, :] = -8.0 * (jnp.maximum(-lam, 0.0) + jnp.log1p(jnp.exp(-jnp.abs(lam))))
    pv_ref[6:10, :] = cw_ref[...].astype(F32)
    wide_ref[0:1, :] = wide_row(bg_ref)
    wide_ref[1:2, :] = wide_row(bu_ref)
    pos_row = seg_ref[0:1, aligned(w * tokens, tokens)].astype(F32)
    pos_cols = jnp.broadcast_to(pos_row, (128, tokens)).T.astype(jnp.int32)
    for k in range(pos_ref.shape[1] // 128):
        pos_ref[:, k * 128:(k + 1) * 128] = pos_cols
    own.wait()
    for copy in copies:
        copy.wait_recv()
    total = jnp.zeros((rows, 1), F32)
    for j in range(nw):
        vals = xbuf[j].astype(F32)
        total = total + jnp.sum(vals * vals, axis=1, keepdims=True)
    my_rows = aligned(c * rows, rows)
    for j in range(nw):
        cols = slice(j * part, (j + 1) * part)
        xown[:, cols] = xbuf[j]
        pars[:, cols] = pbufs[j]
        nall[my_rows, cols] = rms(xbuf[j].astype(F32), total, width, pbufs[j, 0:1])
    begin, middle, end = ring_gather(nall, c, nc, rows, ns, nr)
    begin()
    for copy in copies:
        copy.wait_send()
    send_on_and_next(0)
    middle()
    end()

    ready(0)

    def u_tile(cols, weight):
        u = jnp.dot(nall[...], weight, preferred_element_type=F32) + pv_ref[0:1, cols]
        ubuf[pl.ds(HALO, tokens), cols] = u.astype(BF16).astype(F32)

    column_tiles(wx_all, u_tile)
    hsend[...] = ubuf[pl.ds(tokens, HALO), :].astype(BF16)
    halo = remote(hsend, hrecv, hs.at[0], hr.at[0], wd=shifted(w, 1, nw))
    halo.start()
    send_on_and_next(1)
    ready(1)

    def y_tile(cols, weight):
        y = jnp.dot(nall[...], weight, preferred_element_type=F32) + pv_ref[1:2, cols]
        ybuf[:, cols] = jax.nn.gelu(y, approximate=True).astype(BF16)

    column_tiles(wy_all, y_tile)
    halo.wait()
    ubuf[pl.ds(0, HALO), :] = hrecv[...].astype(F32)
    blocks, bw = rg_ref.shape[0], rg_ref.shape[1]

    def gate_block(j, carry):
        cols = aligned(j * bw, bw)
        pos = pos_ref[...]
        conv = pv_ref[2:3, cols] + ubuf[pl.ds(HALO, tokens), cols] * pv_ref[6:7, cols]
        for k in range(1, 4):
            conv = conv + jnp.where(pos >= k, ubuf[pl.ds(HALO - k, tokens), cols], 0.0) * pv_ref[6 + k:7 + k, cols]
        conv = conv.astype(BF16)
        rate = jax.nn.sigmoid(jnp.dot(conv, rg_ref[j], preferred_element_type=F32) + pv_ref[3:4, cols])
        inflow = jax.nn.sigmoid(jnp.dot(conv, ig_ref[j], preferred_element_type=F32) + pv_ref[4:5, cols])
        log_a = rate * pv_ref[5:6, cols]
        a = jnp.exp(log_a)
        z = 2.0 * log_a
        series = 1.0 + z * (1.0 / 8.0)
        for k in range(7, 1, -1):
            series = 1.0 + z * series * (1.0 / k)
        gap = jnp.maximum(jnp.where(z > -0.5, -z * series, 1.0 - a * a), 0.0)
        root = jnp.where(gap > 0.0, gap * lax.rsqrt(jnp.where(gap > 0.0, gap, 1.0)), 0.0)
        reset = pos == 0
        abuf[:, cols] = jnp.where(reset, 0.0, a)
        bbuf[:, cols] = jnp.where(reset, 1.0, root) * inflow * conv.astype(F32)
        return carry

    lax.fori_loop(0, blocks, gate_block, 0)
    send_on(2)

    sub = lax.broadcasted_iota(jnp.int32, (TILE, chans), 0)

    def scan_tile(i, carry):
        a_in, h_in = carry
        at = aligned(i * TILE, TILE)
        a, b = abuf[at, :], bbuf[at, :]
        for d in (1, 2, 4):
            keep = sub >= d
            b = b + a * jnp.where(keep, pltpu.roll(b, d, 0), 0.0)
            a = a * jnp.where(keep, pltpu.roll(a, d, 0), 1.0)
        h = b + a * h_in
        a = a * a_in
        abuf[at, :] = a
        bbuf[at, :] = h
        return jnp.broadcast_to(a[TILE - 1:], a.shape), jnp.broadcast_to(h[TILE - 1:], h.shape)

    a_tot, h_tot = lax.fori_loop(0, tokens // TILE, scan_tile, (jnp.ones((TILE, chans), F32), jnp.zeros((TILE, chans), F32)))
    tot[w] = jnp.where(sub < TILE // 2, a_tot, h_tot)
    copies = []
    for d in range(1, nw):
        copies.append(remote(tot.at[w], tot.at[w], ts.at[d], tr.at[d], wd=shifted(w, d, nw)))
    for copy in copies:
        copy.start()
    send_own(3)
    for copy in copies:
        copy.wait_recv()
    h_in = jnp.zeros((1, chans), F32)
    for s in range(nw):
        h_in = jnp.where(s < w, tot[s, 0:1] * h_in + tot[s, TILE - 1:], h_in)
    for j in range(blocks):
        cols = slice(j * bw, (j + 1) * bw)
        hidden = bbuf[:, cols] + abuf[:, cols] * h_in[:, cols]
        mixed[:, cols] = (hidden * ybuf[:, cols].astype(F32)).astype(BF16)
    for copy in copies:
        copy.wait_send()

    ready(2)
    first, second, third, drain = ring_sums(c, nc, rows, pbuf, sbuf, far_r, far_l, near_r, near_l, as_, ar)

    def o_load(j, slot):
        return pltpu.make_async_copy(wo_all.at[aligned(j * chans, chans)], ctile.at[slot, pl.ds(0, chans)], csem.at[slot])

    o_load(0, 0).start()

    def o_step(k, carry):
        slot = lax.rem(k, 2)

        @pl.when(k + 1 < nw)
        def _():
            o_load(k + 1, 1 - slot).start()

        o_load(k, slot).wait()
        first(k, jnp.dot(mixed[...], ctile[slot, pl.ds(0, chans), :], preferred_element_type=F32))
        return carry

    def o_second(k, carry):
        second(k)
        return carry

    lax.fori_loop(0, nw, o_step, 0)
    lax.fori_loop(0, nw, o_second, 0)
    send_on_and_next(3)
    total = jnp.zeros((rows, 1), F32)
    for k in range(nw):
        cols = slice(k * part, (k + 1) * part)
        vals = xown[:, cols].astype(F32) + third(k) + pars[1:2, cols]
        res[:, cols] = vals
        total = total + jnp.sum(vals * vals, axis=1, keepdims=True)
    for k in range(nw):
        cols = slice(k * part, (k + 1) * part)
        mall[my_rows, cols] = rms(res[:, cols], total, width, pars[2:3, cols])
    begin, middle, end = ring_gather(mall, c, nc, rows, ms, mr)
    begin()

    def o_drain(k, carry):
        drain(k)
        return carry

    lax.fori_loop(0, nw, o_drain, 0)
    middle()
    end()

    ready(3)

    def g_tile(cols, weight):
        g = jnp.dot(mall[...], weight, preferred_element_type=F32) + wide_ref[0:1, cols]
        gbuf[:, cols] = jax.nn.gelu(g, approximate=True)

    column_tiles(wg_all, g_tile)
    send_on_and_next(4)
    ready(4)

    def i_tile(cols, weight):
        u = jnp.dot(mall[...], weight, preferred_element_type=F32) + wide_ref[1:2, cols]
        inner[:, cols] = (gbuf[:, cols] * u).astype(BF16)

    column_tiles(wu_all, i_tile)

    first, second, third, drain = ring_sums(c, nc, rows, pbuf, sbuf, far_r, far_l, near_r, near_l, ds, dr)
    right, left = shifted(c, 1, nc), shifted(c, -1, nc)
    half = rows // 2
    depth = wd.shape[0]

    targets = [w, mate, back_w, beside(lead, 1), fore_w, beside(nx - lead, 1), far_w, member(2, 1)]
    sources = [w, mate, fore_w, beside(lead, 1), back_w, beside(nx - lead, 1), far_w, member(2, 1)]

    def block_of(d):
        return targets[d]

    def source_of(d):
        return sources[d]

    down, _, keep, part_copy = stream(5)

    def rows_at(owner, group, at=0, size=rows):
        return aligned((owner * nc + group) * rows + at, size)

    def hop(d):
        return remote(osend.at[d], fin.at[rows_at(w, c)], os_.at[d], or_.at[d], wd=block_of(d))

    def spread(d):
        piece = fin.at[rows_at(source_of(d), c)]
        return (remote(piece, piece, fs.at[0, d], fr.at[0, d], ch=right), remote(piece, piece, fs.at[1, d], fr.at[1, d], ch=left))

    def relay(d):
        from_left = fin.at[rows_at(source_of(d), left, 0, half)]
        from_right = fin.at[rows_at(source_of(d), right, half, half)]
        return (remote(from_left, from_left, fs.at[2, d], fr.at[2, d], ch=right), remote(from_right, from_right, fs.at[3, d], fr.at[3, d], ch=left))

    def finish(e):
        cols = aligned(block_of(e) * part, part)
        done = (res[:, cols] + third(e) + pars[3:4, cols]).astype(BF16)

        if e == 0:
            fin[rows_at(w, c), :] = done
        else:
            osend[e] = done
            hop(e).start()

    def share(e):
        if e > 0:
            hop(e).wait_recv()
        for copy in spread(e):
            copy.start()

    def pass_on(e):
        for copy, onward in zip(spread(e), relay(e)):
            copy.wait_recv()
            onward.start()

    def store(e):
        at = aligned(source_of(e) * tokens, tokens)
        return pltpu.make_async_copy(fin.at[at], out_ref.at[at], outsem.at[e])

    def complete(e):
        for copy in relay(e):
            copy.wait_recv()
        store(e).start()

    def fetch(d):
        return pltpu.make_async_copy(wd_all.at[aligned(block_of(d) * depth, depth)], ctile.at[d % 2], csem.at[d % 2])

    def multiply(d):
        fetch(d).wait()
        first(d, jnp.dot(inner[...], ctile[d % 2], preferred_element_type=F32))

    def take(*indices):
        for k in indices:
            down(k).wait_recv()

    def relay_piece(t):
        for k in range(2):
            part_copy(k, t).wait_recv()
            part_copy(2 + k, t).start()

    keep().wait()
    fetch(0).start()
    take(4)
    fetch(1).start()
    multiply(0)
    multiply(1)
    down(2).start()
    down(3).start()
    take(0, 1)
    fetch(2).start()
    down(7).start()
    down(8).start()
    second(0)
    second(1)
    multiply(2)
    finish(0)
    share(0)
    finish(1)
    take(7, 8)
    fetch(3).start()
    share(1)
    second(2)
    multiply(3)
    take(2)
    down(9).start()
    for t in range(PIECES - 1):
        for k in range(2):
            part_copy(k, t).start()
    pass_on(0)
    pass_on(1)
    finish(2)
    second(3)
    finish(3)
    take(3)
    fetch(4).start()
    down(10).start()
    multiply(4)
    for k in range(2):
        part_copy(k, PIECES - 1).start()
    take(9, 10)
    fetch(5).start()
    second(4)
    multiply(5)
    share(2)
    share(3)
    finish(4)
    second(5)
    for t in range(PIECES - 1):
        relay_piece(t)
    finish(5)
    relay_piece(PIECES - 1)
    fetch(6).start()
    pass_on(2)
    multiply(6)
    for t in range(PIECES):
        for k in range(2):
            part_copy(2 + k, t).wait_recv()
    fetch(7).start()
    share(4)
    multiply(7)
    pass_on(3)
    second(6)
    share(5)
    second(7)
    pass_on(4)
    finish(6)
    pass_on(5)
    finish(7)
    share(6)
    for e in range(4):
        complete(e)
    share(7)
    pass_on(6)
    complete(4)
    complete(5)
    pass_on(7)
    complete(6)
    complete(7)
    for e in range(nw):
        for copy in spread(e) + relay(e):
            copy.wait_send()
        drain(e)
        if e > 0:
            hop(e).wait_send()
    for i in range(len(weights)):
        copy, _, _, part_copy = stream(i)
        last = i + 1 == len(weights)
        for k in range(13):
            if not (last and k in (5, 6, 11, 12)):
                copy(k).wait_send()
        if last:
            for kind in range(4):
                for t in range(PIECES):
                    part_copy(kind, t).wait_send()
    for k in range(nw):
        store(k).wait()


def dma(*shape):
    return pltpu.SemaphoreType.DMA(shape)


def solution(mesh):
    nw = mesh.shape['wd']
    nc = mesh.shape['ch']
    assert nc == 4 and nw == 8
    row_spec = P('dp', 'wd')
    specs = (row_spec, P('dp', None), P('wd'), P('wd', 'ch'), P('ch'), P('wd', 'ch'), P('ch'), P(None, 'ch'), P('ch'), P('ch'), P('ch', None, None), P('ch'), P('ch', None, None), P('ch'), P('ch', 'wd'), P('wd'), P('wd'), P('wd', 'ch'), P('ch'), P('wd', 'ch'), P('ch'), P('ch', 'wd'), P('wd'))
    vm = pl.BlockSpec(memory_space=VMEM)
    anywhere = pl.BlockSpec(memory_space=ANY)

    def local_layer(resid_in, seg_pos, gain_temporal, w_x, bias_x, w_y, bias_y, conv_w, conv_bias, lam_param, rgate_w, rgate_b, igate_w, igate_b, w_o, bias_o, gain_mlp, w_g, bias_g, w_u, bias_u, w_d, bias_d):
        tokens, part = resid_in.shape
        width = part * nw
        span = tokens // nw
        rows = span // nc
        chans = w_x.shape[1]
        wide = w_g.shape[1]
        bw = rgate_w.shape[1]
        assert seg_pos.shape[0] == 1

        def landing(arr):
            return jax.ShapeDtypeStruct((arr.shape[0] * nw, arr.shape[1]), arr.dtype)

        stream = (w_x, w_y, w_o, w_g, w_u, w_d)
        scratch = [
            VMEM((nw, rows, part), BF16), VMEM((nw, 8, part), F32), VMEM((16, chans), F32), VMEM((span, bw), jnp.int32), VMEM((8, wide), F32), VMEM((rows, width), BF16), VMEM((8, width), F32),
            VMEM((span, width), BF16), VMEM((span, width), BF16), VMEM((2, width, bw), BF16), VMEM((2, wide, part), BF16),
            VMEM((part, wide), BF16), VMEM((wide, part), BF16),
            VMEM((span + HALO, chans), F32), VMEM((HALO, chans), BF16), VMEM((HALO, chans), BF16), VMEM((span, chans), BF16),
            VMEM((span, chans), F32), VMEM((span, chans), F32), VMEM((nw, TILE, chans), F32), VMEM((span, chans), BF16),
            VMEM((span, wide), F32), VMEM((span, wide), BF16), VMEM((rows, width), F32),
            VMEM((nw, span, part), F32), VMEM((nw, span, part), BF16), VMEM((nw, rows // 2, part), BF16), VMEM((nw, rows // 2, part), BF16),
            VMEM((nw, rows, part), BF16), VMEM((nw, rows, part), BF16), VMEM((nw, rows, part), BF16), VMEM((tokens, part), BF16),
            dma(4), dma(2), dma(2), dma(nw), dma(nw), dma(nw), dma(nw), dma(nw), dma(6), dma(6), dma(1), dma(1), dma(nw), dma(nw),
            dma(4, nw), dma(4, nw), dma(6), dma(6), dma(4, nw), dma(4, nw), dma(nw), dma(nw), dma(4, nw), dma(4, nw),
            dma(len(stream), 13), dma(len(stream), 13), dma(4, PIECES), dma(4, PIECES),
        ]
        return pl.pallas_call(
            functools.partial(layer_kernel, nw, nc), name='layer',
            out_shape=(jax.ShapeDtypeStruct((tokens, part), BF16),) + tuple(landing(arr) for arr in stream),
            in_specs=[anywhere] + [vm] + [anywhere] * 6 + [vm] * 15, out_specs=(anywhere,) * 7, scratch_shapes=scratch,
            compiler_params=pltpu.CompilerParams(vmem_limit_bytes=VMEM_LIMIT, collective_id=0, has_side_effects=True),
        )(resid_in, seg_pos, *stream, gain_temporal, bias_o, gain_mlp, bias_d, bias_x, bias_y, conv_bias, rgate_b, igate_b, lam_param, conv_w, rgate_w, igate_w, bias_g, bias_u)[0]

    return jax.shard_map(local_layer, mesh=mesh, in_specs=specs, out_specs=row_spec, check_vma=False)
```
